256 devices in a mesh: dom: 256 (over y, x, z, core).
Axes of the slice: x: 4, y: 4, z: 8, core: 2. Of those that a mesh axis runs over, the one named last changes fastest.
Arguments:
- displacement: float32 [8, 3, 524288], P(None, None, 'dom'), may hold values from -1.5 to 1.5
- adjoint_disp: float32 [8, 3, 524288], P(None, None, 'dom'), may hold values from -1.5 to 1.5
- pressure: float32 [8, 524288], P(None, 'dom'), may hold values from -3 to 3
- adjoint_pressure: float32 [8, 524288], P(None, 'dom'), may hold values from -3 to 3
- youngs: float32 [524288], P('dom'), may hold values from 0.5 to 2
- permeability: float32 [524288], P('dom'), may hold values from 0.3 to 3
- stiffness: float32 [24, 24], replicated
- send_nodes: int32 [8, 32768], P(None, 'dom'), may hold values from 0 to 2047
- send_cells: int32 [8, 32768], P(None, 'dom'), may hold values from 0 to 2047
- elem_nodes: int32 [8, 524288], P(None, 'dom'), may hold values from 0 to 3071, as said below
- inner_faces: int32 [2, 1572864], P(None, 'dom'), may hold values from 0 to 2047
- cross_faces: int32 [2, 262144], P(None, 'dom'), may hold values from 0 to 2047, as said below
Outputs:
- grad_log_youngs: float32 [524288], P('dom')
- grad_log_perm: float32 [524288], P('dom')
The draws below stay inside these ranges and needn't reach their ends.
Inputs may be any that keep to these rules, and one draw needn't show every extreme that they name: `send_nodes`: entries refer to the partition's own nodes; block j of partition c is read by partition c - o_j, with o as in the reference program. `send_cells`: entries refer to the partition's own cells; block j of partition c is read by partition c - o_j. `elem_nodes`: local numbering as in the reference program; a ghost entry j * 128 + g always has d + o_j on the axis. The first 1536 elements of each partition name only its own nodes; corner 0 of each of the last 512 is a ghost node. `cross_faces`: row 0 is an own cell; row 1 is j * 128 + g with d + o_j always on the axis. `inner_faces`: both rows name cells of the same partition.
All inputs are finite; a program needn't handle non-finite values.
Results may differ from the reference program's by a relative error of at most 0.0003.
Values sent between devices are 32-bit elements; how exact they have to be, the bound alone decides.
A program may use at most 192 MiB of HBM per device.

```python
import math
import jax
import jax.numpy as jnp
from jax import lax

EL = 2048
STEPS = 8
NB = 8
DOFS = 24
NL = 2048
EB = 512
GN = 128
GC = 128
FI = 6144
FX = 1024
NODES = 524288
CELLS = 524288
N_DOM = 256


OFFSETS = (1, -1, 2, -2, 4, -4, 8, -8)


def valid_slots(key, device):
    offsets = jnp.array(OFFSETS, dtype=jnp.int32)
    slot_id = jax.random.randint(key, device.shape, 0, NB, dtype=jnp.int32)
    target = device + offsets[slot_id]
    inside = (target >= 0) & (target < N_DOM)
    return jnp.where(inside, slot_id, slot_id ^ 1).astype(jnp.int32)


def draw_elem_nodes(key, part):
    key_list = jax.random.split(jax.random.fold_in(key, 11), 4)
    total_rows = EL * N_DOM
    device = jnp.arange(total_rows, dtype=jnp.int32) // EL
    element = jnp.arange(total_rows, dtype=jnp.int32) % EL
    own_node = jax.random.randint(key_list[0], (8, total_rows), 0, NL, dtype=jnp.int32)
    slot_id = valid_slots(key_list[1], jnp.broadcast_to(device[None, :], (8, total_rows)))
    row_id = jax.random.randint(key_list[2], (8, total_rows), 0, GN, dtype=jnp.int32)
    ghost_node = NL + slot_id * GN + row_id
    chosen = (jax.random.randint(key_list[3], (8, total_rows), 0, 2, dtype=jnp.int32) == 1) | (jnp.arange(8, dtype=jnp.int32)[:, None] == 0)
    edge_rows = element >= EL - EB
    return jnp.where(edge_rows[None, :] & chosen, ghost_node, own_node).astype(jnp.int32)


def draw_cross_faces(key, part):
    key_list = jax.random.split(jax.random.fold_in(key, 23), 3)
    total_rows = FX * N_DOM
    device = jnp.arange(total_rows, dtype=jnp.int32) // FX
    own_cell = jax.random.randint(key_list[0], (total_rows,), 0, EL, dtype=jnp.int32)
    slot_id = valid_slots(key_list[1], device)
    row_id = jax.random.randint(key_list[2], (total_rows,), 0, GC, dtype=jnp.int32)
    return jnp.stack([own_cell, slot_id * GC + row_id]).astype(jnp.int32)


def draw_stiffness(key, part):
    inner_key = jax.random.fold_in(key, 37)
    base = jax.random.normal(inner_key, (DOFS, DOFS), jnp.float32)
    return (jnp.eye(DOFS, dtype=jnp.float32) + 0.5 * (base + base.T) / math.sqrt(2.0 * DOFS)).astype(jnp.float32)


def place_ends(entries, own_key, smallest, top_value):
    place = [jax.random.randint(jax.random.fold_in(own_key, axis), (), 0, length) for axis, length in enumerate(entries.shape)]
    longest = entries.shape.index(max(entries.shape))
    neighbour = place[:longest] + [(place[longest] + 1) % entries.shape[longest]] + place[longest + 1:]
    return entries.at[tuple(place)].set(smallest).at[tuple(neighbour)].set(top_value)


def levels(stream_key, shape, pieces, least, top_value):
    gain, own = 1.0, jax.random.fold_in(stream_key, 6)
    for position, shards_of in pieces:
        draws = jnp.exp(jax.random.uniform(jax.random.fold_in(own, position), (shards_of,), jnp.float32, least / len(pieces), top_value / len(pieces)))
        gain = gain * jnp.repeat(draws, shape[position] // shards_of).reshape([-1 if axis == position else 1 for axis in range(len(shape))])
    return gain


def noise(rng, extent, deviation, bound, cuts=(), kind=jnp.bfloat16):
    values = deviation * jax.random.normal(rng, extent, jnp.float32)
    if cuts:
        values = values * levels(rng, extent, cuts, -0.22, 0.18)
    return jnp.clip(values, -bound, bound).astype(kind)


def setup_inputs(seed: int = 0) -> dict:
    splits = jax.random.split(jax.random.key(seed), 13)
    return {
        "displacement": noise(splits[0], (STEPS, 3, NODES), 0.25, 1.5, ((2, 256),), jnp.float32),
        "adjoint_disp": noise(splits[1], (STEPS, 3, NODES), 0.25, 1.5, ((2, 256),), jnp.float32),
        "pressure": noise(splits[2], (STEPS, CELLS), 0.5, 3.0, ((1, 256),), jnp.float32),
        "adjoint_pressure": noise(splits[3], (STEPS, CELLS), 0.5, 3.0, ((1, 256),), jnp.float32),
        "youngs": jnp.clip(jnp.exp(math.log(2.0) - 1.3862944 * jax.random.uniform(splits[4], (CELLS,), jnp.float32) ** levels(splits[4], (CELLS,), ((0, 256),), -0.2, 0.2)), 0.5, 2.0),
        "permeability": jnp.clip(jnp.exp(math.log(3.0) - 2.3025851 * jax.random.uniform(splits[5], (CELLS,), jnp.float32) ** levels(splits[5], (CELLS,), ((0, 256),), -0.2, 0.2)), 0.3, 3.0),
        "stiffness": draw_stiffness(jax.random.fold_in(splits[12], 71), 0),
        "send_nodes": place_ends(jax.random.randint(splits[7], (NB, GN * N_DOM), 0, NL), jax.random.fold_in(splits[7], 1), 0, NL - 1).astype(jnp.int32),
        "send_cells": place_ends(jax.random.randint(splits[8], (NB, GC * N_DOM), 0, EL), jax.random.fold_in(splits[8], 1), 0, EL - 1).astype(jnp.int32),
        "elem_nodes": draw_elem_nodes(jax.random.fold_in(splits[12], 71), 0),
        "inner_faces": place_ends(jax.random.randint(splits[10], (2, FI * N_DOM), 0, EL), jax.random.fold_in(splits[10], 1), 0, EL - 1).astype(jnp.int32),
        "cross_faces": draw_cross_faces(jax.random.fold_in(splits[12], 71), 0),
    }


OFFSETS = (1, -1, 2, -2, 4, -4, 8, -8)


def face_terms(press_a, press_b, adj_a, adj_b, perm_a, perm_b):
    product = jnp.sum((press_a - press_b) * (adj_a - adj_b), axis=0)
    denominator = (perm_a + perm_b) * (perm_a + perm_b)
    common = 2.0 * perm_a * perm_b * product / denominator
    return common * perm_b, common * perm_a


def reference(displacement, adjoint_disp, pressure, adjoint_pressure, youngs, permeability, stiffness, send_nodes, send_cells, elem_nodes, inner_faces, cross_faces):
    offsets = jnp.array(OFFSETS, dtype=jnp.int32)
    node_blocks = send_nodes.reshape(NB, N_DOM, GN)

    def one_device(device):
        sources = jnp.clip(device + offsets, 0, N_DOM - 1).astype(jnp.int32)
        ghost_nodes = node_blocks[jnp.arange(NB, dtype=jnp.int32), sources] + sources[:, None] * NL
        table = jnp.concatenate([device * NL + jnp.arange(NL, dtype=jnp.int32), ghost_nodes.reshape(-1).astype(jnp.int32)])
        connect = lax.dynamic_slice_in_dim(elem_nodes, (device * EL).astype(jnp.int32), EL, 1)
        global_nodes = table[connect]
        forward = displacement[:, :, global_nodes].reshape(STEPS, DOFS, EL)
        adjoint = adjoint_disp[:, :, global_nodes].reshape(STEPS, DOFS, EL)
        weighted = jnp.einsum("ab,tbe->tae", stiffness, forward, precision=lax.Precision.HIGHEST)
        strain = jnp.sum(adjoint * weighted, axis=(0, 1))
        modulus = lax.dynamic_slice_in_dim(youngs, (device * EL).astype(jnp.int32), EL, 0)
        return -modulus * strain

    grad_youngs = lax.map(one_device, jnp.arange(N_DOM, dtype=jnp.int32)).reshape(-1)

    inner_base = (jnp.arange(FI * N_DOM, dtype=jnp.int32) // FI) * EL
    face_a = inner_faces[0] + inner_base
    face_b = inner_faces[1] + inner_base
    cross_dev = jnp.arange(FX * N_DOM, dtype=jnp.int32) // FX
    slot_id = (cross_faces[1] // GC).astype(jnp.int32)
    row_id = (cross_faces[1] % GC).astype(jnp.int32)
    source = jnp.clip(cross_dev + offsets[slot_id], 0, N_DOM - 1).astype(jnp.int32)
    cross_a = cross_dev * EL + cross_faces[0]
    cross_b = source * EL + send_cells[slot_id, source * GC + row_id]

    term_a, term_b = face_terms(pressure[:, face_a], pressure[:, face_b], adjoint_pressure[:, face_a], adjoint_pressure[:, face_b], permeability[face_a], permeability[face_b])
    shared_a, shared_b = face_terms(pressure[:, cross_a], pressure[:, cross_b], adjoint_pressure[:, cross_a], adjoint_pressure[:, cross_b], permeability[cross_a], permeability[cross_b])
    gradient = jnp.zeros((CELLS,), jnp.float32)
    gradient = gradient.at[face_a].add(term_a).at[face_b].add(term_b)
    gradient = gradient.at[cross_a].add(shared_a).at[cross_b].add(shared_b)
    return grad_youngs, gradient
```

```python
import functools

import jax
import jax.numpy as jnp
from jax import lax
from jax.experimental import pallas as pl
from jax.experimental.pallas import tpu as pltpu
from jax.sharding import PartitionSpec as P

OFFSETS = (1, -1, 2, -2, 4, -4, 8, -8)
MESH = pl.DeviceIdType.MESH
F32 = jnp.float32
BF16 = jnp.bfloat16
LANES = 128
STEPS = 8
OWN = 16
NB = 8
CELL_ROWS = 24
NODE_ROWS = 48
CELL_BLOCKS = 6
INNER_BLOCKS = 12
ALL_BLOCKS = 16


def take(source, lanes):
    return jnp.take_along_axis(source, lanes, axis=1, mode="promise_in_bounds")


def pick(values, bits):
    if len(values) == 1:
        return values[0]()
    half = len(values) // 2
    top = bits[half.bit_length() - 1]
    low = pick(values[:half], bits)
    high = pick(values[half:], bits)
    return jnp.where(top, high, low)


def spread(ref, row, column):
    return jnp.broadcast_to(ref[row : row + 1, column : column + LANES], (8, LANES))


def bit_masks(chunk, count):
    return [(chunk & (1 << bit)) != 0 for bit in range(count)]


def own_rows(ref, row, lanes, bits):
    return pick(
        [lambda h=h: take(spread(ref, row, h * LANES), lanes) for h in range(OWN)],
        bits,
    )


def own_perm(ref, lanes, bits):
    return pick([lambda h=h: take(spread(ref, h, 0), lanes) for h in range(OWN)], bits)


def ghost_rows(ref, row, pitch, lanes, bits):
    return pick(
        [lambda j=j: take(spread(ref, j * pitch + row, 0), lanes) for j in range(NB)],
        bits,
    )


def split(value):
    high = value.astype(BF16).astype(F32)
    return high, value - high


def contract_lanes(left, right):
    return lax.dot_general(
        left, right, (((1,), (1,)), ((), ())), preferred_element_type=F32
    )


def scatter_rows(index, value_ref, rows, index_row):
    chunk_iota = lax.broadcasted_iota(jnp.int32, (rows, LANES), 0)
    lane_iota = lax.broadcasted_iota(jnp.int32, (LANES, LANES), 0)
    left, right = [], []
    for s in range(8):
        where = index_row(s)
        value = jnp.broadcast_to(value_ref[s : s + 1, :], (rows, LANES))
        chunk = jnp.broadcast_to(where >> 7, (rows, LANES))
        left.append(jnp.where(chunk == chunk_iota, value, 0.0))
        lane = jnp.broadcast_to(where & 127, (LANES, LANES))
        right.append(jnp.where(lane == lane_iota, 1.0, 0.0).astype(BF16))
    wide = jnp.concatenate(left, axis=1)
    high, low = split(wide)
    both = jnp.concatenate([high, low], axis=0).astype(BF16)
    summed = contract_lanes(both, jnp.concatenate(right, axis=1))
    return summed[:rows] + summed[rows:]


def face_common(perm_a, perm_b, product):
    both = perm_a + perm_b
    return 2.0 * perm_a * perm_b * product / (both * both)


def kernel(
    count,
    disp_ref,
    adj_ref,
    press_ref,
    apress_ref,
    youngs_ref,
    perm_ref,
    stiff_ref,
    send_nodes_ref,
    send_cells_ref,
    elem_ref,
    inner_ref,
    cross_ref,
    gy_ref,
    gp_ref,
    cells_out,
    nodes_out,
    cells_in,
    nodes_in,
    back_out,
    back_in,
    term_a_ref,
    term_b_ref,
    cell_send,
    cell_recv,
    node_send,
    node_recv,
    back_send,
    back_recv,
):
    me = lax.axis_index("dom")

    def at(offset):
        return (lax.rem(me + (offset + count), count),)

    barrier = pltpu.get_barrier_semaphore()
    for offset in OFFSETS:
        pl.semaphore_signal(barrier, inc=1, device_id=at(offset), device_id_type=MESH)

    index = send_cells_ref[...]
    lanes, bits = index & 127, bit_masks(index >> 7, 4)
    for t in range(STEPS):
        cells_out[pl.ds(t, NB, stride=CELL_ROWS), :] = own_rows(press_ref, t, lanes, bits)
        cells_out[pl.ds(STEPS + t, NB, stride=CELL_ROWS), :] = own_rows(
            apress_ref, t, lanes, bits
        )
    for r in range(2 * STEPS, CELL_ROWS):
        if r == 2 * STEPS:
            permeability = own_perm(perm_ref, lanes, bits)
        cells_out[pl.ds(r, NB, stride=CELL_ROWS), :] = permeability
    index = send_nodes_ref[...]
    lanes, bits = index & 127, bit_masks(index >> 7, 4)
    for r in range(24):
        nodes_out[pl.ds(r, NB, stride=NODE_ROWS), :] = own_rows(disp_ref, r, lanes, bits)
        nodes_out[pl.ds(24 + r, NB, stride=NODE_ROWS), :] = own_rows(
            adj_ref, r, lanes, bits
        )

    pl.semaphore_wait(barrier, NB)

    def cell_copy(j):
        return pltpu.make_async_remote_copy(
            src_ref=cells_out.at[pl.ds(j * CELL_ROWS, CELL_ROWS)],
            dst_ref=cells_in.at[pl.ds(j * CELL_ROWS, CELL_ROWS)],
            send_sem=cell_send.at[j],
            recv_sem=cell_recv.at[j],
            device_id=at(-OFFSETS[j]),
            device_id_type=MESH,
        )

    def node_copy(j):
        return pltpu.make_async_remote_copy(
            src_ref=nodes_out.at[pl.ds(j * NODE_ROWS, NODE_ROWS)],
            dst_ref=nodes_in.at[pl.ds(j * NODE_ROWS, NODE_ROWS)],
            send_sem=node_send.at[j],
            recv_sem=node_recv.at[j],
            device_id=at(-OFFSETS[j]),
            device_id_type=MESH,
        )

    def back_copy(j):
        return pltpu.make_async_remote_copy(
            src_ref=back_out,
            dst_ref=back_in.at[pl.ds(8 * j, 8)],
            send_sem=back_send.at[j],
            recv_sem=back_recv.at[j],
            device_id=at(OFFSETS[j]),
            device_id_type=MESH,
        )

    for j in range(NB):
        cell_copy(j).start()
    for j in range(NB):
        node_copy(j).start()

    def inner_faces(block, gradient):
        base = pl.multiple_of(block * 16, 16)
        ends = []
        for side in range(2):
            index = inner_ref[pl.ds(base + side, 8, stride=2), :]
            lanes, bits = index & 127, bit_masks(index >> 7, 4)
            ends.append(
                (
                    [own_rows(press_ref, t, lanes, bits) for t in range(STEPS)],
                    [own_rows(apress_ref, t, lanes, bits) for t in range(STEPS)],
                    own_perm(perm_ref, lanes, bits),
                )
            )
        (pa, qa, ka), (pb, qb, kb) = ends
        product = sum((pa[t] - pb[t]) * (qa[t] - qb[t]) for t in range(STEPS))
        common = face_common(ka, kb, product)
        term_a_ref[...] = common * kb
        term_b_ref[...] = common * ka
        for side, term_ref in enumerate((term_a_ref, term_b_ref)):
            gradient = gradient + scatter_rows(
                None,
                term_ref,
                OWN,
                lambda s: inner_ref[pl.ds(base + 2 * s + side, 1), :],
            )
        return gradient

    gradient = lax.fori_loop(0, CELL_BLOCKS, inner_faces, jnp.zeros((OWN, LANES), F32))

    stiff_high, stiff_low = split(stiff_ref[...])
    stiff = jnp.concatenate([stiff_high, stiff_low, stiff_high], axis=1).astype(BF16)

    def elements(block, ghosts):
        column = pl.multiple_of(block * LANES, LANES)
        index = elem_ref[:, pl.ds(column, LANES)]
        lanes, chunk = index & 127, index >> 7
        bits = bit_masks(chunk, 4)
        outside = chunk >= OWN

        def corner_rows(ref, row, ghost_row):
            value = own_rows(ref, row, lanes, bits)
            if ghosts:
                value = jnp.where(
                    outside, ghost_rows(nodes_in, ghost_row, NODE_ROWS, lanes, bits), value
                )
            return value

        total = jnp.zeros((8, LANES), F32)
        for t in range(STEPS):
            forward = jnp.concatenate(
                [corner_rows(disp_ref, 8 * c + t, 8 * c + t) for c in range(3)], axis=0
            )
            adjoint = [corner_rows(adj_ref, 8 * c + t, 24 + 8 * c + t) for c in range(3)]
            high, low = split(forward)
            stacked = jnp.concatenate([high, high, low], axis=0).astype(BF16)
            weighted = jnp.dot(stiff, stacked, preferred_element_type=F32)
            for c in range(3):
                total = total + adjoint[c] * weighted[8 * c : 8 * c + 8]
        strain = jnp.sum(total, axis=0, keepdims=True)
        gy_ref[pl.ds(block, 1), :] = -youngs_ref[pl.ds(block, 1), :] * strain

    @pl.loop(0, INNER_BLOCKS)
    def _(block):
        elements(block, False)

    for j in range(NB):
        cell_copy(j).wait_recv()
    index = cross_ref[pl.ds(0, 8, stride=2), :]
    lanes, bits = index & 127, bit_masks(index >> 7, 4)
    index = cross_ref[pl.ds(1, 8, stride=2), :]
    ghost_lanes, ghost_bits = index & 127, bit_masks(index >> 7, 3)

    def ghost(row):
        return ghost_rows(cells_in, row, CELL_ROWS, ghost_lanes, ghost_bits)

    product = jnp.zeros((8, LANES), F32)
    for t in range(STEPS):
        product = product + (own_rows(press_ref, t, lanes, bits) - ghost(t)) * (
            own_rows(apress_ref, t, lanes, bits) - ghost(STEPS + t)
        )
    perm_a, perm_b = own_perm(perm_ref, lanes, bits), ghost(2 * STEPS)
    common = face_common(perm_a, perm_b, product)
    term_a_ref[...] = common * perm_b
    term_b_ref[...] = common * perm_a
    back_out[...] = scatter_rows(
        None, term_b_ref, NB, lambda s: cross_ref[2 * s + 1 : 2 * s + 2, :]
    )
    gradient = gradient + scatter_rows(
        None, term_a_ref, OWN, lambda s: cross_ref[2 * s : 2 * s + 1, :]
    )
    for j in range(NB):
        back_copy(j).start()

    for j in range(NB):
        node_copy(j).wait_recv()

    @pl.loop(INNER_BLOCKS, ALL_BLOCKS)
    def _(block):
        elements(block, True)

    for j in range(NB):
        back_copy(j).wait_recv()
    term_a_ref[...] = back_in[pl.ds(0, NB, stride=9), :]
    gp_ref[...] = gradient + scatter_rows(
        None, term_a_ref, OWN, lambda s: send_cells_ref[s : s + 1, :]
    )
    for j in range(NB):
        cell_copy(j).wait_send()
        node_copy(j).wait_send()
        back_copy(j).wait_send()


def on_device(
    displacement,
    adjoint_disp,
    pressure,
    adjoint_pressure,
    youngs,
    permeability,
    stiffness,
    send_nodes,
    send_cells,
    elem_nodes,
    inner_faces,
    cross_faces,
):
    count = lax.axis_size("dom")

    def components(value):
        return value.transpose(1, 0, 2).reshape(24, -1)

    def interleaved(value):
        return value.reshape(2, -1, LANES).transpose(1, 0, 2).reshape(-1, LANES)

    vmem = pl.BlockSpec(memory_space=pltpu.VMEM)
    grad_youngs, grad_perm = pl.pallas_call(
        functools.partial(kernel, count),
        out_shape=(
            jax.ShapeDtypeStruct((OWN, LANES), F32),
            jax.ShapeDtypeStruct((OWN, LANES), F32),
        ),
        in_specs=[vmem] * 12,
        out_specs=(vmem, vmem),
        scratch_shapes=[
            pltpu.VMEM((NB * CELL_ROWS, LANES), F32),
            pltpu.VMEM((NB * NODE_ROWS, LANES), F32),
            pltpu.VMEM((NB * CELL_ROWS, LANES), F32),
            pltpu.VMEM((NB * NODE_ROWS, LANES), F32),
            pltpu.VMEM((NB, LANES), F32),
            pltpu.VMEM((NB * 9, LANES), F32),
            pltpu.VMEM((8, LANES), F32),
            pltpu.VMEM((8, LANES), F32),
        ]
        + [pltpu.SemaphoreType.DMA((NB,))] * 6,
        compiler_params=pltpu.CompilerParams(collective_id=0, has_side_effects=True),
    )(
        components(displacement),
        components(adjoint_disp),
        pressure,
        adjoint_pressure,
        youngs.reshape(OWN, LANES),
        permeability.reshape(OWN, LANES),
        stiffness,
        send_nodes,
        send_cells,
        elem_nodes,
        interleaved(inner_faces),
        interleaved(cross_faces),
    )
    return grad_youngs.reshape(-1), grad_perm.reshape(-1)


def solution(mesh):
    in_specs = (
        P(None, None, "dom"),
        P(None, None, "dom"),
        P(None, "dom"),
        P(None, "dom"),
        P("dom"),
        P("dom"),
        P(),
        P(None, "dom"),
        P(None, "dom"),
        P(None, "dom"),
        P(None, "dom"),
        P(None, "dom"),
    )
    return jax.shard_map(
        on_device,
        mesh=mesh,
        in_specs=in_specs,
        out_specs=(P("dom"), P("dom")),
        check_vma=False,
    )
```

```python
import functools

import jax
import jax.numpy as jnp
from jax import lax
from jax.experimental import pallas as pl
from jax.experimental.pallas import tpu as pltpu
from jax.sharding import PartitionSpec as P

OFFSETS = (1, -1, 2, -2, 4, -4, 8, -8)
MESH = pl.DeviceIdType.MESH
F32 = jnp.float32
BF16 = jnp.bfloat16
LANES = 128
STEPS = 8
OWN = 16
NB = 8
CELL_ROWS = 24
NODE_ROWS = 48
CELL_BLOCKS = 6
INNER_BLOCKS = 12
ALL_BLOCKS = 16
WIDE = 256
OWN_GROUPS = 8
GHOST_GROUPS = 4
GROUP = 4
PITCH = 56
SPAN = 16
CROSS_AT = 3


def take(source, lanes):
    return jnp.take_along_axis(source, lanes, axis=1, mode="promise_in_bounds")


def pick(values, bits):
    if len(values) == 1:
        return values[0]()
    half = len(values) // 2
    top = bits[half.bit_length() - 1]
    low = pick(values[:half], bits)
    high = pick(values[half:], bits)
    return jnp.where(top, high, low)


def spread(ref, row, column):
    return jnp.broadcast_to(ref[row : row + 1, column : column + LANES], (8, LANES))


def bit_masks(chunk, count):
    return [(chunk & (1 << bit)) != 0 for bit in range(count)]


def own_rows(ref, row, lanes, bits):
    return pick(
        [lambda h=h: take(spread(ref, row, h * LANES), lanes) for h in range(OWN)],
        bits,
    )


def own_perm(ref, lanes, bits):
    return pick([lambda h=h: take(spread(ref, h, 0), lanes) for h in range(OWN)], bits)


def ghost_rows(ref, row, pitch, lanes, bits):
    return pick(
        [lambda j=j: take(spread(ref, j * pitch + row, 0), lanes) for j in range(NB)],
        bits,
    )


def split(value):
    high = value.astype(BF16).astype(F32)
    return high, value - high


def contract_lanes(left, right):
    return lax.dot_general(
        left, right, (((1,), (1,)), ((), ())), preferred_element_type=F32
    )


def scatter_rows(value_ref, rows, index_row):
    chunk_iota = lax.broadcasted_iota(jnp.int32, (rows, LANES), 0)
    lane_iota = lax.broadcasted_iota(jnp.int32, (LANES, LANES), 0)
    left, right = [], []
    for s in range(8):
        where = index_row(s)
        value = jnp.broadcast_to(value_ref[s : s + 1, :], (rows, LANES))
        chunk = jnp.broadcast_to(where >> 7, (rows, LANES))
        left.append(jnp.where(chunk == chunk_iota, value, 0.0))
        lane = jnp.broadcast_to(where & 127, (LANES, LANES))
        right.append(jnp.where(lane == lane_iota, 1.0, 0.0).astype(BF16))
    wide = jnp.concatenate(left, axis=1)
    high, low = split(wide)
    both = jnp.concatenate([high, low], axis=0).astype(BF16)
    summed = contract_lanes(both, jnp.concatenate(right, axis=1))
    return summed[:rows] + summed[rows:]


def table_rows(value):
    high = value.astype(BF16)
    low = (value - high.astype(F32)).astype(BF16)
    return jnp.concatenate([high, low], axis=1)


def lookup(table_ref, groups, indices):
    place = lax.broadcasted_iota(jnp.int32, (WIDE, LANES), 0)
    columns = []
    for index in indices:
        column = jnp.broadcast_to((index & (WIDE - 1))[:1], (WIDE, LANES))
        columns.append(jnp.where(column == place, 1.0, 0.0).astype(BF16))
    once = jnp.concatenate(columns, axis=1)
    found = jnp.dot(
        table_ref[: groups * NODE_ROWS, :],
        jnp.concatenate([once, once], axis=0),
        preferred_element_type=F32,
    )
    results = []
    for n, index in enumerate(indices):
        group = index >> 8
        bits = bit_masks(group, 3)

        def piece(h, k):
            row = h * NODE_ROWS + 8 * k
            return found[row : row + 8, n * LANES : (n + 1) * LANES]

        pieces = []
        for k in range(NODE_ROWS // 8):
            value = pick([lambda h=h: piece(h, k) for h in range(OWN_GROUPS)], bits)
            if groups > OWN_GROUPS:
                outside = pick(
                    [lambda h=h: piece(OWN_GROUPS + h, k) for h in range(GHOST_GROUPS)],
                    bits,
                )
                value = jnp.where(group >= OWN_GROUPS, outside, value)
            pieces.append(value)
        results.append(pieces)
    return results


def face_common(perm_a, perm_b, product):
    both = perm_a + perm_b
    return 2.0 * perm_a * perm_b * product / (both * both)


def kernel(
    count,
    disp_ref,
    adj_ref,
    press_ref,
    apress_ref,
    youngs_ref,
    perm_ref,
    stiff_ref,
    send_nodes_ref,
    send_cells_ref,
    elem_ref,
    inner_ref,
    cross_ref,
    gy_ref,
    gp_ref,
    cells_out,
    nodes_out,
    cells_in,
    nodes_in,
    back_out,
    back_in,
    term_a_ref,
    term_b_ref,
    table_ref,
    state_ref,
    gradient_ref,
    cell_send,
    cell_recv,
    node_send,
    node_recv,
    back_send,
    back_recv,
):
    me = lax.axis_index("dom")

    def on_axis(offset):
        return (me + offset >= 0) & (me + offset < count)

    def at(offset):
        return (me + offset,)

    barrier = pltpu.get_barrier_semaphore()
    neighbours = 0
    for offset in OFFSETS:

        @pl.when(on_axis(offset))
        def _():
            pl.semaphore_signal(barrier, inc=1, device_id=at(offset), device_id_type=MESH)

        neighbours = neighbours + on_axis(offset).astype(jnp.int32)

    index = send_cells_ref[...]
    lanes, bits = index & 127, bit_masks(index >> 7, 4)
    for t in range(STEPS):
        cells_out[pl.ds(t, NB, stride=CELL_ROWS), :] = own_rows(press_ref, t, lanes, bits)
        cells_out[pl.ds(STEPS + t, NB, stride=CELL_ROWS), :] = own_rows(
            apress_ref, t, lanes, bits
        )
    for r in range(2 * STEPS, CELL_ROWS):
        if r == 2 * STEPS:
            permeability = own_perm(perm_ref, lanes, bits)
        cells_out[pl.ds(r, NB, stride=CELL_ROWS), :] = permeability
    for h in range(OWN_GROUPS):
        columns = slice(h * WIDE, (h + 1) * WIDE)
        table_ref[h * NODE_ROWS : (h + 1) * NODE_ROWS, :] = table_rows(
            jnp.concatenate([disp_ref[:, columns], adj_ref[:, columns]], axis=0)
        )
    for first in range(0, NB, GROUP):
        rows = [
            jnp.broadcast_to(send_nodes_ref[j : j + 1, :], (8, LANES))
            for j in range(first, first + GROUP)
        ]
        for j, pieces in zip(range(first, first + GROUP), lookup(table_ref, OWN_GROUPS, rows)):
            for k, value in enumerate(pieces):
                row = j * NODE_ROWS + 8 * k
                nodes_out[row : row + 8, :] = value

    for j in range(NB):

        @pl.when(jnp.logical_not(on_axis(OFFSETS[j])))
        def _():
            rows = slice(j * NODE_ROWS, (j + 1) * NODE_ROWS)
            nodes_in[rows, :] = jnp.zeros((NODE_ROWS, LANES), F32)

        @pl.when(jnp.logical_not(on_axis(-OFFSETS[j])))
        def _():
            back_in[8 * j : 8 * j + 8, :] = jnp.zeros((8, LANES), F32)

    def cell_copy(j):
        return pltpu.make_async_remote_copy(
            src_ref=cells_out.at[pl.ds(j * CELL_ROWS, CELL_ROWS)],
            dst_ref=cells_in.at[pl.ds(j * CELL_ROWS, CELL_ROWS)],
            send_sem=cell_send.at[j],
            recv_sem=cell_recv.at[j],
            device_id=at(-OFFSETS[j]),
            device_id_type=MESH,
        )

    def node_copy(j):
        return pltpu.make_async_remote_copy(
            src_ref=nodes_out.at[pl.ds(j * NODE_ROWS, NODE_ROWS)],
            dst_ref=nodes_in.at[pl.ds(j * NODE_ROWS, NODE_ROWS)],
            send_sem=node_send.at[j],
            recv_sem=node_recv.at[j],
            device_id=at(-OFFSETS[j]),
            device_id_type=MESH,
        )

    def back_copy(j):
        return pltpu.make_async_remote_copy(
            src_ref=back_out,
            dst_ref=back_in.at[pl.ds(8 * j, 8)],
            send_sem=back_send.at[j],
            recv_sem=back_recv.at[j],
            device_id=at(OFFSETS[j]),
            device_id_type=MESH,
        )

    def each(offset_sign, action):
        for j in reversed(range(NB)):
            pl.when(on_axis(offset_sign * OFFSETS[j]))(lambda j=j: action(j))

    def send_states():
        pl.semaphore_wait(barrier, neighbours)
        each(-1, lambda j: cell_copy(j).start())
        each(-1, lambda j: node_copy(j).start())

    def inner_faces(block):
        base = pl.multiple_of(block * 16, 16)
        ends = []
        for side in range(2):
            index = inner_ref[pl.ds(base + side, 8, stride=2), :]
            lanes, bits = index & 127, bit_masks(index >> 7, 4)
            ends.append(
                (
                    [own_rows(press_ref, t, lanes, bits) for t in range(STEPS)],
                    [own_rows(apress_ref, t, lanes, bits) for t in range(STEPS)],
                    own_perm(perm_ref, lanes, bits),
                )
            )
        (pa, qa, ka), (pb, qb, kb) = ends
        product = sum((pa[t] - pb[t]) * (qa[t] - qb[t]) for t in range(STEPS))
        common = face_common(ka, kb, product)
        term_a_ref[...] = common * kb
        term_b_ref[...] = common * ka
        gradient = gradient_ref[...]
        for side, term_ref in enumerate((term_a_ref, term_b_ref)):
            gradient = gradient + scatter_rows(
                term_ref,
                OWN,
                lambda s: inner_ref[pl.ds(base + 2 * s + side, 1), :],
            )
        gradient_ref[...] = gradient

    stiff_high, stiff_low = split(stiff_ref[...])
    stiff = jnp.concatenate([stiff_high, stiff_low, stiff_high], axis=1).astype(BF16)

    def elements(block, groups):
        column = pl.multiple_of(block * LANES, LANES)
        for first in range(0, 8, GROUP):
            rows = [
                jnp.broadcast_to(elem_ref[n : n + 1, pl.ds(column, LANES)], (8, LANES))
                for n in range(first, first + GROUP)
            ]
            for n, pieces in zip(range(first, first + GROUP), lookup(table_ref, groups, rows)):
                for k, value in enumerate(pieces):
                    row = n * PITCH + 8 * k
                    state_ref[row : row + 8, :] = value
        total = jnp.zeros((8, LANES), F32)
        for t in range(STEPS):
            forward = jnp.concatenate(
                [state_ref[pl.ds(8 * c + t, 8, stride=PITCH), :] for c in range(3)], axis=0
            )
            high, low = split(forward)
            stacked = jnp.concatenate([high, high, low], axis=0).astype(BF16)
            weighted = jnp.dot(stiff, stacked, preferred_element_type=F32)
            for c in range(3):
                adjoint = state_ref[pl.ds(24 + 8 * c + t, 8, stride=PITCH), :]
                total = total + adjoint * weighted[8 * c : 8 * c + 8]
        strain = jnp.sum(total, axis=0, keepdims=True)
        gy_ref[pl.ds(block, 1), :] = -youngs_ref[pl.ds(block, 1), :] * strain

    def shared_faces():
        each(1, lambda j: cell_copy(j).wait_recv())
        index = cross_ref[pl.ds(0, 8, stride=2), :]
        lanes, bits = index & 127, bit_masks(index >> 7, 4)
        index = cross_ref[pl.ds(1, 8, stride=2), :]
        ghost_lanes, ghost_bits = index & 127, bit_masks(index >> 7, 3)

        def ghost(row):
            return ghost_rows(cells_in, row, CELL_ROWS, ghost_lanes, ghost_bits)

        product = jnp.zeros((8, LANES), F32)
        for t in range(STEPS):
            product = product + (own_rows(press_ref, t, lanes, bits) - ghost(t)) * (
                own_rows(apress_ref, t, lanes, bits) - ghost(STEPS + t)
            )
        perm_a, perm_b = own_perm(perm_ref, lanes, bits), ghost(2 * STEPS)
        common = face_common(perm_a, perm_b, product)
        term_a_ref[...] = common * perm_b
        term_b_ref[...] = common * perm_a
        back_out[...] = scatter_rows(
            term_b_ref, NB, lambda s: cross_ref[2 * s + 1 : 2 * s + 2, :]
        )
        gradient_ref[...] += scatter_rows(
            term_a_ref, OWN, lambda s: cross_ref[2 * s : 2 * s + 1, :]
        )
        each(1, lambda j: back_copy(j).start())

    gradient_ref[...] = jnp.zeros((OWN, LANES), F32)
    early = lax.rem(me, SPAN) < SPAN // 2
    send_at = jnp.where(early, CELL_BLOCKS, 0)
    cross_at = jnp.where(early, CELL_BLOCKS, CROSS_AT)

    @pl.loop(0, CELL_BLOCKS + 1)
    def _(step):
        pl.when(step == send_at)(send_states)
        pl.when(step == cross_at)(shared_faces)

        @pl.when(step < CELL_BLOCKS)
        def _():
            elements(2 * step, OWN_GROUPS)
            elements(2 * step + 1, OWN_GROUPS)
            inner_faces(step)

    each(1, lambda j: node_copy(j).wait_recv())
    for h in range(GHOST_GROUPS):
        row = (OWN_GROUPS + h) * NODE_ROWS
        ghosts = [
            nodes_in[j * NODE_ROWS : (j + 1) * NODE_ROWS, :] for j in (2 * h, 2 * h + 1)
        ]
        table_ref[row : row + NODE_ROWS, :] = table_rows(jnp.concatenate(ghosts, axis=1))

    @pl.loop(INNER_BLOCKS, ALL_BLOCKS)
    def _(block):
        elements(block, OWN_GROUPS + GHOST_GROUPS)

    each(-1, lambda j: back_copy(j).wait_recv())
    term_a_ref[...] = back_in[pl.ds(0, NB, stride=9), :]
    gp_ref[...] = gradient_ref[...] + scatter_rows(
        term_a_ref, OWN, lambda s: send_cells_ref[s : s + 1, :]
    )
    each(-1, lambda j: cell_copy(j).wait_send())
    each(-1, lambda j: node_copy(j).wait_send())
    each(1, lambda j: back_copy(j).wait_send())


def on_device(
    displacement,
    adjoint_disp,
    pressure,
    adjoint_pressure,
    youngs,
    permeability,
    stiffness,
    send_nodes,
    send_cells,
    elem_nodes,
    inner_faces,
    cross_faces,
):
    count = lax.axis_size("dom")

    def components(value):
        return value.transpose(1, 0, 2).reshape(24, -1)

    def interleaved(value):
        return value.reshape(2, -1, LANES).transpose(1, 0, 2).reshape(-1, LANES)

    vmem = pl.BlockSpec(memory_space=pltpu.VMEM)
    grad_youngs, grad_perm = pl.pallas_call(
        functools.partial(kernel, count),
        out_shape=(
            jax.ShapeDtypeStruct((OWN, LANES), F32),
            jax.ShapeDtypeStruct((OWN, LANES), F32),
        ),
        in_specs=[vmem] * 12,
        out_specs=(vmem, vmem),
        scratch_shapes=[
            pltpu.VMEM((NB * CELL_ROWS, LANES), F32),
            pltpu.VMEM((NB * NODE_ROWS, LANES), F32),
            pltpu.VMEM((NB * CELL_ROWS, LANES), F32),
            pltpu.VMEM((NB * NODE_ROWS, LANES), F32),
            pltpu.VMEM((NB, LANES), F32),
            pltpu.VMEM((NB * 9, LANES), F32),
            pltpu.VMEM((8, LANES), F32),
            pltpu.VMEM((8, LANES), F32),
            pltpu.VMEM(((OWN_GROUPS + GHOST_GROUPS) * NODE_ROWS, 2 * WIDE), BF16),
            pltpu.VMEM((8 * PITCH, LANES), F32),
            pltpu.VMEM((OWN, LANES), F32),
        ]
        + [pltpu.SemaphoreType.DMA((NB,))] * 6,
        compiler_params=pltpu.CompilerParams(collective_id=0, has_side_effects=True),
    )(
        components(displacement),
        components(adjoint_disp),
        pressure,
        adjoint_pressure,
        youngs.reshape(OWN, LANES),
        permeability.reshape(OWN, LANES),
        stiffness,
        send_nodes,
        send_cells,
        elem_nodes,
        interleaved(inner_faces),
        interleaved(cross_faces),
    )
    return grad_youngs.reshape(-1), grad_perm.reshape(-1)


def solution(mesh):
    in_specs = (
        P(None, None, "dom"),
        P(None, None, "dom"),
        P(None, "dom"),
        P(None, "dom"),
        P("dom"),
        P("dom"),
        P(),
        P(None, "dom"),
        P(None, "dom"),
        P(None, "dom"),
        P(None, "dom"),
        P(None, "dom"),
    )
    return jax.shard_map(
        on_device,
        mesh=mesh,
        in_specs=in_specs,
        out_specs=(P("dom"), P("dom")),
        check_vma=False,
    )
```

```python
import functools

import jax
import jax.numpy as jnp
from jax import lax
from jax.experimental import pallas as pl
from jax.experimental.pallas import tpu as pltpu
from jax.sharding import PartitionSpec as P

OFFSETS = (1, -1, 2, -2, 4, -4, 8, -8)
MESH = pl.DeviceIdType.MESH
F32 = jnp.float32
BF16 = jnp.bfloat16
LANES = 128
STEPS = 8
OWN = 16
NB = 8
CELL_ROWS = 16
NODE_ROWS = 48
CELL_BLOCKS = 6
INNER_BLOCKS = 12
EDGE_BLOCKS = 4
WIDE = 256
OWN_GROUPS = 8
GHOST_GROUPS = 4
GROUP = 4
PITCH = 56
SPAN = 16
ROW = 64
EARLIEST = 4
CROSS_AFTER = 5


def take(source, lanes):
    return jnp.take_along_axis(source, lanes, axis=1, mode="promise_in_bounds")


def pick(values, bits):
    if len(values) == 1:
        return values[0]()
    half = len(values) // 2
    top = bits[half.bit_length() - 1]
    low = pick(values[:half], bits)
    high = pick(values[half:], bits)
    return jnp.where(top, high, low)


def wide(row):
    return jnp.broadcast_to(row, (8, LANES))


def bit_masks(chunk, count):
    return [(chunk & (1 << bit)) != 0 for bit in range(count)]


def own_rows(ref, row, lanes, bits):
    return pick(
        [
            lambda h=h: take(wide(ref[row : row + 1, h * LANES : (h + 1) * LANES]), lanes)
            for h in range(OWN)
        ],
        bits,
    )


def own_perm(ref, lanes, bits):
    return pick(
        [lambda h=h: take(wide(ref[h : h + 1, :]), lanes) for h in range(OWN)], bits
    )


def ghost_rows(rows, lanes, bits):
    return pick([lambda j=j: take(wide(rows(j)), lanes) for j in range(NB)], bits)


def split(value):
    high = value.astype(BF16).astype(F32)
    return high, value - high


def small(column):
    column = column.astype(F32)
    return jnp.concatenate([column, column], axis=0).astype(BF16)


def lane_marks(place_ref, index_row):
    one, zero = jnp.ones((16, LANES), BF16), jnp.zeros((16, LANES), BF16)
    columns = []
    for s in range(8):
        lane = small(wide(index_row(s)) & (LANES - 1))
        columns.append(
            jnp.concatenate(
                [
                    jnp.where(lane == place_ref[row : row + 16, :], one, zero)
                    for row in range(0, LANES, 16)
                ],
                axis=0,
            )
        )
    return jnp.concatenate(columns, axis=1)


def scatter_rows(marks, value_ref, rows, index_row):
    chunk_iota = lax.broadcasted_iota(jnp.int32, (rows, LANES), 0)
    left = []
    for s in range(8):
        value = jnp.broadcast_to(value_ref[s : s + 1, :], (rows, LANES))
        chunk = jnp.concatenate([wide(index_row(s)) >> 7] * (rows // 8), axis=0)
        left.append(jnp.where(chunk == chunk_iota, value, 0.0))
    high, low = split(jnp.concatenate(left, axis=1))
    summed = lax.dot_general(
        jnp.concatenate([high, low], axis=0).astype(BF16),
        marks,
        (((1,), (1,)), ((), ())),
        preferred_element_type=F32,
    )
    return summed[:rows] + summed[rows:]


def fill_table(table_ref, row, value):
    high = value.astype(BF16)
    low = (value - high.astype(F32)).astype(BF16)
    for half in range(2):
        columns = slice(half * LANES, (half + 1) * LANES)
        table_ref[half, row : row + NODE_ROWS, :] = high[:, columns]
        table_ref[2 + half, row : row + NODE_ROWS, :] = low[:, columns]


def mark(place_ref, once_ref, slot, indices):
    one, zero = jnp.ones((16, LANES), BF16), jnp.zeros((16, LANES), BF16)
    for n, index in enumerate(indices):
        column = small(index & (WIDE - 1))
        for row in range(0, WIDE, 16):
            match = column == place_ref[row : row + 16, :]
            once_ref[slot, n, row : row + 16, :] = jnp.where(match, one, zero)


def lookup(table_ref, first, groups, once_ref, slot, indices):
    once = jnp.concatenate([once_ref[slot, n] for n in range(len(indices))], axis=1)
    rows = slice(first * NODE_ROWS, (first + groups) * NODE_ROWS)
    found = sum(
        jnp.dot(
            jnp.concatenate([table_ref[plane, rows, :], table_ref[plane + 1, rows, :]], axis=1),
            once,
            preferred_element_type=F32,
        )
        for plane in (0, 2)
    )
    results = []
    for n, index in enumerate(indices):
        bits = bit_masks(index >> 8, 3)

        def piece(h, k):
            row = h * NODE_ROWS + 8 * k
            return found[row : row + 8, n * LANES : (n + 1) * LANES]

        results.append(
            [
                pick([lambda h=h: piece(h, k) for h in range(groups)], bits)
                for k in range(NODE_ROWS // 8)
            ]
        )
    return results


def face_common(perm_a, perm_b, product):
    both = perm_a + perm_b
    return 2.0 * perm_a * perm_b * product / (both * both)


def kernel(
    count,
    disp_hbm,
    adj_hbm,
    press_hbm,
    apress_hbm,
    youngs_hbm,
    perm_hbm,
    stiff_hbm,
    send_nodes_hbm,
    send_cells_hbm,
    elem_hbm,
    inner_hbm,
    cross_hbm,
    gy_ref,
    gp_ref,
    disp_ref,
    adj_ref,
    press_ref,
    apress_ref,
    youngs_ref,
    perm_ref,
    stiff_ref,
    send_nodes_ref,
    send_cells_ref,
    elem_ref,
    inner_ref,
    cross_ref,
    cells_out,
    perms_out,
    nodes_out,
    cells_in,
    perms_in,
    nodes_in,
    back_out,
    back_in,
    term_a_ref,
    term_b_ref,
    edge_ref,
    face_ref,
    back_marks_ref,
    table_ref,
    place_ref,
    once_ref,
    edge_once_ref,
    state_ref,
    edge_state_ref,
    gradient_ref,
    cell_send,
    cell_recv,
    perm_send,
    perm_recv,
    node_send,
    node_recv,
    back_send,
    back_recv,
    stage_sem,
):
    me = lax.axis_index("dom")

    def on_axis(offset):
        return (me + offset >= 0) & (me + offset < count)

    barrier = pltpu.get_barrier_semaphore()
    neighbours = 0
    for offset in OFFSETS:

        @pl.when(on_axis(offset))
        def _():
            pl.semaphore_signal(
                barrier, inc=1, device_id=(me + offset,), device_id_type=MESH
            )

        neighbours = neighbours + on_axis(offset).astype(jnp.int32)

    staged = (
        (send_cells_hbm, send_cells_ref),
        (press_hbm, press_ref),
        (apress_hbm, apress_ref),
        (perm_hbm, perm_ref),
        (send_nodes_hbm, send_nodes_ref),
        (disp_hbm, disp_ref),
        (adj_hbm, adj_ref),
        (elem_hbm, elem_ref),
        (inner_hbm, inner_ref),
        (stiff_hbm, stiff_ref),
        (youngs_hbm, youngs_ref),
        (cross_hbm, cross_ref),
    )
    stages = [
        pltpu.make_async_copy(source, target, stage_sem.at[i])
        for i, (source, target) in enumerate(staged)
    ]
    for stage in stages:
        stage.start()

    def send(source, target, send_sem, recv_sem, j, offset):
        return pltpu.make_async_remote_copy(
            src_ref=source,
            dst_ref=target,
            send_sem=send_sem.at[j],
            recv_sem=recv_sem.at[j],
            device_id=(me + offset,),
            device_id_type=MESH,
        )

    def cell_copy(j):
        rows = pl.ds(j * CELL_ROWS, CELL_ROWS)
        return send(cells_out.at[rows], cells_in.at[rows], cell_send, cell_recv, j, -OFFSETS[j])

    def perm_copy(j):
        return send(perms_out.at[j], perms_in.at[j], perm_send, perm_recv, j, -OFFSETS[j])

    def node_copy(j):
        rows = pl.ds(j * NODE_ROWS, NODE_ROWS)
        return send(nodes_out.at[rows], nodes_in.at[rows], node_send, node_recv, j, -OFFSETS[j])

    def back_copy(j):
        return send(back_out.at[j], back_in.at[j], back_send, back_recv, j, OFFSETS[j])

    def each(sign, action):
        for j in reversed(range(NB)):
            pl.when(on_axis(sign * OFFSETS[j]))(lambda j=j: action(j))

    place = lax.broadcasted_iota(jnp.int32, (WIDE, LANES), 0)
    place_ref[...] = place.astype(F32).astype(BF16)
    gradient_ref[...] = jnp.zeros((OWN, LANES), F32)
    term_a_ref[...] = jnp.zeros((8, LANES), F32)
    term_b_ref[...] = jnp.zeros((8, LANES), F32)
    state_ref[...] = jnp.zeros(state_ref.shape, F32)
    for j in range(NB):

        @pl.when(jnp.logical_not(on_axis(OFFSETS[j])))
        def _():
            rows = slice(j * NODE_ROWS, (j + 1) * NODE_ROWS)
            nodes_in[rows, :] = jnp.zeros((NODE_ROWS, LANES), F32)

        @pl.when(jnp.logical_not(on_axis(-OFFSETS[j])))
        def _():
            back_in[j] = jnp.zeros((1, LANES), F32)

    for stage in stages:
        stage.wait()

    index = send_cells_ref[...]
    lanes, bits = index & 127, bit_masks(index >> 7, 4)
    for t in range(STEPS):
        cells_out[pl.ds(t, NB, stride=CELL_ROWS), :] = own_rows(press_ref, t, lanes, bits)
        cells_out[pl.ds(STEPS + t, NB, stride=CELL_ROWS), :] = own_rows(
            apress_ref, t, lanes, bits
        )
    permeability = own_perm(perm_ref, lanes, bits)
    for j in range(NB):
        perms_out[j] = permeability[j : j + 1, :]
    for h in range(OWN_GROUPS):
        columns = slice(h * WIDE, (h + 1) * WIDE)
        fill_table(
            table_ref,
            h * NODE_ROWS,
            jnp.concatenate([disp_ref[:, columns], adj_ref[:, columns]], axis=0),
        )
    for first in range(0, NB, GROUP):
        rows = [wide(send_nodes_ref[j : j + 1, :]) for j in range(first, first + GROUP)]
        slot = first // GROUP
        mark(place_ref, once_ref, slot, rows)
        found = lookup(table_ref, 0, OWN_GROUPS, once_ref, slot, rows)
        for j, pieces in zip(range(first, first + GROUP), found):
            for k, value in enumerate(pieces):
                row = j * NODE_ROWS + 8 * k
                nodes_out[row : row + 8, :] = value

    def send_states():
        pl.semaphore_wait(barrier, neighbours)

        def start_cells(j):
            cell_copy(j).start()
            perm_copy(j).start()

        each(-1, start_cells)
        each(-1, lambda j: node_copy(j).start())

    def gather_inner(block):
        base = pl.multiple_of(block * 16, 16)
        ends = []
        for side in range(2):
            index = inner_ref[pl.ds(base + side, 8, stride=2), :]
            lanes, bits = index & 127, bit_masks(index >> 7, 4)
            ends.append(
                (
                    [own_rows(press_ref, t, lanes, bits) for t in range(STEPS)],
                    [own_rows(apress_ref, t, lanes, bits) for t in range(STEPS)],
                    own_perm(perm_ref, lanes, bits),
                )
            )
        (pa, qa, ka), (pb, qb, kb) = ends
        product = sum((pa[t] - pb[t]) * (qa[t] - qb[t]) for t in range(STEPS))
        common = face_common(ka, kb, product)
        term_a_ref[...] = common * kb
        term_b_ref[...] = common * ka

    def scatter_inner(block):
        base = pl.multiple_of(block * 16, 16)
        gradient = gradient_ref[...]
        for side, term_ref in enumerate((term_a_ref, term_b_ref)):
            index_row = lambda s: inner_ref[pl.ds(base + 2 * s + side, 1), :]
            marks = lane_marks(place_ref, index_row)
            gradient = gradient + scatter_rows(marks, term_ref, OWN, index_row)
        gradient_ref[...] = gradient

    stiff_high, stiff_low = split(stiff_ref[...])
    stiff = jnp.concatenate([stiff_high, stiff_low, stiff_high], axis=1).astype(BF16)

    def element_rows(block, first):
        column = pl.multiple_of(block * LANES, LANES)
        return [
            wide(elem_ref[n : n + 1, pl.ds(column, LANES)]) for n in range(first, first + GROUP)
        ]

    def own_states(block, once, states, slot):
        for first in range(0, 8, GROUP):
            rows = element_rows(block, first)
            part = 2 * slot + first // GROUP
            mark(place_ref, once, part, rows)
            found = lookup(table_ref, 0, OWN_GROUPS, once, part, rows)
            for n, pieces in zip(range(first, first + GROUP), found):
                for k, value in enumerate(pieces):
                    row = n * PITCH + 8 * k
                    states[slot, row : row + 8, :] = value

    def ghost_states(block, slot):
        for first in range(0, 8, GROUP):
            rows = element_rows(block, first)
            part = 2 * slot + first // GROUP
            found = lookup(table_ref, OWN_GROUPS, GHOST_GROUPS, edge_once_ref, part, rows)
            for n, index, pieces in zip(range(first, first + GROUP), rows, found):
                outside = index >= OWN * LANES
                for k, value in enumerate(pieces):
                    row = n * PITCH + 8 * k
                    edge_state_ref[slot, row : row + 8, :] = jnp.where(
                        outside, value, edge_state_ref[slot, row : row + 8, :]
                    )

    def strain(block, states, slot):
        total = jnp.zeros((8, LANES), F32)
        for t in range(0, STEPS, 2):
            forward = jnp.concatenate(
                [
                    jnp.concatenate(
                        [states[slot, pl.ds(8 * c + u, 8, stride=PITCH), :] for c in range(3)],
                        axis=0,
                    )
                    for u in (t, t + 1)
                ],
                axis=1,
            )
            high, low = split(forward)
            stacked = jnp.concatenate([high, high, low], axis=0).astype(BF16)
            weighted = jnp.dot(stiff, stacked, preferred_element_type=F32)
            for u in range(2):
                for c in range(3):
                    adjoint = states[slot, pl.ds(24 + 8 * c + t + u, 8, stride=PITCH), :]
                    total = total + adjoint * weighted[
                        8 * c : 8 * c + 8, u * LANES : (u + 1) * LANES
                    ]
        summed = jnp.sum(total, axis=0, keepdims=True)
        gy_ref[pl.ds(block, 1), :] = -youngs_ref[pl.ds(block, 1), :] * summed

    def shared_faces():
        index = cross_ref[pl.ds(0, 8, stride=2), :]
        lanes, bits = index & 127, bit_masks(index >> 7, 4)
        for t in range(STEPS):
            face_ref[t] = own_rows(press_ref, t, lanes, bits)
            face_ref[STEPS + t] = own_rows(apress_ref, t, lanes, bits)
        perm_a = own_perm(perm_ref, lanes, bits)
        index = cross_ref[pl.ds(1, 8, stride=2), :]
        ghost_lanes, ghost_bits = index & 127, bit_masks(index >> 7, 3)

        def ghost(row):
            return ghost_rows(
                lambda j: cells_in[j * CELL_ROWS + row : j * CELL_ROWS + row + 1, :],
                ghost_lanes,
                ghost_bits,
            )

        ghost_index = lambda s: cross_ref[2 * s + 1 : 2 * s + 2, :]
        own_index = lambda s: cross_ref[2 * s : 2 * s + 1, :]
        back_marks_ref[...] = lane_marks(place_ref, ghost_index)

        def wait_cells(j):
            cell_copy(j).wait_recv()
            perm_copy(j).wait_recv()

        each(1, wait_cells)
        product = jnp.zeros((8, LANES), F32)
        for t in range(STEPS):
            product = product + (face_ref[t] - ghost(t)) * (
                face_ref[STEPS + t] - ghost(STEPS + t)
            )
        perm_b = ghost_rows(lambda j: perms_in[j], ghost_lanes, ghost_bits)
        common = face_common(perm_a, perm_b, product)
        edge_ref[0] = common * perm_b
        edge_ref[1] = common * perm_a
        returned = scatter_rows(back_marks_ref[...], edge_ref.at[1], NB, ghost_index)
        for j in range(NB):
            back_out[j] = returned[j : j + 1, :]
        each(1, lambda j: back_copy(j).start())
        gradient_ref[...] += scatter_rows(
            lane_marks(place_ref, own_index), edge_ref.at[0], OWN, own_index
        )

    place_z = lax.rem(me, SPAN) // 2
    early = place_z < SPAN // 4
    row_start = (me >= ROW) & (lax.rem(me, ROW) < SPAN)
    send_at = jnp.where(early, EARLIEST - place_z + row_start.astype(jnp.int32), 0)
    cross_at = jnp.minimum(send_at + CROSS_AFTER, CELL_BLOCKS)

    @pl.loop(0, CELL_BLOCKS)
    def _(step):
        pl.when(step == send_at)(send_states)
        pl.when(step == cross_at)(shared_faces)
        before = jnp.maximum(step - 1, 0)
        strain(2 * before, state_ref, 0)
        strain(2 * before + 1, state_ref, 1)
        scatter_inner(before)
        own_states(2 * step, once_ref, state_ref, 0)
        own_states(2 * step + 1, once_ref, state_ref, 1)
        gather_inner(step)

    strain(INNER_BLOCKS - 2, state_ref, 0)
    strain(INNER_BLOCKS - 1, state_ref, 1)
    scatter_inner(CELL_BLOCKS - 1)
    for slot in range(EDGE_BLOCKS):
        own_states(INNER_BLOCKS + slot, edge_once_ref, edge_state_ref, slot)
    pl.when(send_at == CELL_BLOCKS)(send_states)
    pl.when(cross_at == CELL_BLOCKS)(shared_faces)

    each(1, lambda j: node_copy(j).wait_recv())
    for h in range(GHOST_GROUPS):
        row = (OWN_GROUPS + h) * NODE_ROWS
        ghosts = [
            nodes_in[j * NODE_ROWS : (j + 1) * NODE_ROWS, :] for j in (2 * h, 2 * h + 1)
        ]
        fill_table(table_ref, row, jnp.concatenate(ghosts, axis=1))
    for slot in range(EDGE_BLOCKS):
        ghost_states(INNER_BLOCKS + slot, slot)
    for slot in range(EDGE_BLOCKS):
        strain(INNER_BLOCKS + slot, edge_state_ref, slot)

    cell_index = lambda s: send_cells_ref[s : s + 1, :]
    back_marks_ref[...] = lane_marks(place_ref, cell_index)
    each(-1, lambda j: back_copy(j).wait_recv())
    edge_ref[0] = jnp.concatenate([back_in[j] for j in range(NB)], axis=0)
    gp_ref[...] = gradient_ref[...] + scatter_rows(
        back_marks_ref[...], edge_ref.at[0], OWN, cell_index
    )
    each(-1, lambda j: cell_copy(j).wait_send())
    each(-1, lambda j: perm_copy(j).wait_send())
    each(-1, lambda j: node_copy(j).wait_send())
    each(1, lambda j: back_copy(j).wait_send())


def on_device(
    displacement,
    adjoint_disp,
    pressure,
    adjoint_pressure,
    youngs,
    permeability,
    stiffness,
    send_nodes,
    send_cells,
    elem_nodes,
    inner_faces,
    cross_faces,
):
    count = lax.axis_size("dom")

    def components(value):
        return value.transpose(1, 0, 2).reshape(24, -1)

    def interleaved(value):
        return value.reshape(2, -1, LANES).transpose(1, 0, 2).reshape(-1, LANES)

    vmem = pl.BlockSpec(memory_space=pltpu.VMEM)
    grad_youngs, grad_perm = pl.pallas_call(
        functools.partial(kernel, count),
        out_shape=(
            jax.ShapeDtypeStruct((OWN, LANES), F32),
            jax.ShapeDtypeStruct((OWN, LANES), F32),
        ),
        in_specs=[pl.BlockSpec(memory_space=pltpu.HBM)] * 12,
        out_specs=(vmem, vmem),
        scratch_shapes=[
            pltpu.VMEM((24, OWN * LANES), F32),
            pltpu.VMEM((24, OWN * LANES), F32),
            pltpu.VMEM((STEPS, OWN * LANES), F32),
            pltpu.VMEM((STEPS, OWN * LANES), F32),
            pltpu.VMEM((OWN, LANES), F32),
            pltpu.VMEM((OWN, LANES), F32),
            pltpu.VMEM((24, 24), F32),
            pltpu.VMEM((NB, LANES), jnp.int32),
            pltpu.VMEM((NB, LANES), jnp.int32),
            pltpu.VMEM((8, OWN * LANES), jnp.int32),
            pltpu.VMEM((16 * CELL_BLOCKS, LANES), jnp.int32),
            pltpu.VMEM((16, LANES), jnp.int32),
            pltpu.VMEM((NB * CELL_ROWS, LANES), F32),
            pltpu.VMEM((NB, 1, LANES), F32),
            pltpu.VMEM((NB * NODE_ROWS, LANES), F32),
            pltpu.VMEM((NB * CELL_ROWS, LANES), F32),
            pltpu.VMEM((NB, 1, LANES), F32),
            pltpu.VMEM((NB * NODE_ROWS, LANES), F32),
            pltpu.VMEM((NB, 1, LANES), F32),
            pltpu.VMEM((NB, 1, LANES), F32),
            pltpu.VMEM((8, LANES), F32),
            pltpu.VMEM((8, LANES), F32),
            pltpu.VMEM((2, 8, LANES), F32),
            pltpu.VMEM((2 * STEPS, 8, LANES), F32),
            pltpu.VMEM((LANES, 8 * LANES), BF16),
            pltpu.VMEM((4, (OWN_GROUPS + GHOST_GROUPS) * NODE_ROWS, LANES), BF16),
            pltpu.VMEM((WIDE, LANES), BF16),
            pltpu.VMEM((4, GROUP, WIDE, LANES), BF16),
            pltpu.VMEM((2 * EDGE_BLOCKS, GROUP, WIDE, LANES), BF16),
            pltpu.VMEM((2, 8 * PITCH, LANES), F32),
            pltpu.VMEM((EDGE_BLOCKS, 8 * PITCH, LANES), F32),
            pltpu.VMEM((OWN, LANES), F32),
        ]
        + [pltpu.SemaphoreType.DMA((NB,))] * 8
        + [pltpu.SemaphoreType.DMA((12,))],
        compiler_params=pltpu.CompilerParams(collective_id=0, has_side_effects=True),
    )(
        components(displacement),
        components(adjoint_disp),
        pressure,
        adjoint_pressure,
        youngs.reshape(OWN, LANES),
        permeability.reshape(OWN, LANES),
        stiffness,
        send_nodes,
        send_cells,
        elem_nodes,
        interleaved(inner_faces),
        interleaved(cross_faces),
    )
    return grad_youngs.reshape(-1), grad_perm.reshape(-1)


def solution(mesh):
    in_specs = (
        P(None, None, "dom"),
        P(None, None, "dom"),
        P(None, "dom"),
        P(None, "dom"),
        P("dom"),
        P("dom"),
        P(),
        P(None, "dom"),
        P(None, "dom"),
        P(None, "dom"),
        P(None, "dom"),
        P(None, "dom"),
    )
    return jax.shard_map(
        on_device,
        mesh=mesh,
        in_specs=in_specs,
        out_specs=(P("dom"), P("dom")),
        check_vma=False,
    )
```

```python
import functools

import jax
import jax.numpy as jnp
from jax import lax
from jax.experimental import pallas as pl
from jax.experimental.pallas import tpu as pltpu
from jax.sharding import PartitionSpec as P

OFFSETS = (1, -1, 2, -2, 4, -4, 8, -8)
MESH = pl.DeviceIdType.MESH
F32 = jnp.float32
BF16 = jnp.bfloat16
LANES = 128
STEPS = 8
OWN = 16
NB = 8
CELL_ROWS = 16
NODE_ROWS = 48
CELL_BLOCKS = 6
INNER_BLOCKS = 12
EDGE_BLOCKS = 4
WIDE = 256
OWN_GROUPS = 8
GHOST_GROUPS = 4
GROUP = 4
PITCH = 56
SPAN = 16
ROW = 64
EARLIEST = 4
CROSS_AFTER = 4


def take(source, lanes):
    return jnp.take_along_axis(source, lanes, axis=1, mode="promise_in_bounds")


def pick(values, bits):
    if len(values) == 1:
        return values[0]()
    half = len(values) // 2
    top = bits[half.bit_length() - 1]
    low = pick(values[:half], bits)
    high = pick(values[half:], bits)
    return jnp.where(top, high, low)


def wide(row):
    return jnp.broadcast_to(row, (8, LANES))


def bit_masks(chunk, count):
    return [(chunk & (1 << bit)) != 0 for bit in range(count)]


def own_rows(ref, row, lanes, bits):
    return pick(
        [
            lambda h=h: take(wide(ref[row : row + 1, h * LANES : (h + 1) * LANES]), lanes)
            for h in range(OWN)
        ],
        bits,
    )


def own_perm(ref, lanes, bits):
    return pick(
        [lambda h=h: take(wide(ref[h : h + 1, :]), lanes) for h in range(OWN)], bits
    )


def ghost_rows(rows, lanes, bits):
    return pick([lambda j=j: take(wide(rows(j)), lanes) for j in range(NB)], bits)


def split(value):
    high = value.astype(BF16).astype(F32)
    return high, value - high


def small(column):
    column = column.astype(F32)
    return jnp.concatenate([column, column], axis=0).astype(BF16)


def lane_marks(place_ref, index_row):
    one, zero = jnp.ones((16, LANES), BF16), jnp.zeros((16, LANES), BF16)
    columns = []
    for s in range(8):
        lane = small(wide(index_row(s)) & (LANES - 1))
        columns.append(
            jnp.concatenate(
                [
                    jnp.where(lane == place_ref[row : row + 16, :], one, zero)
                    for row in range(0, LANES, 16)
                ],
                axis=0,
            )
        )
    return jnp.concatenate(columns, axis=1)


def scatter_rows(marks, value_ref, rows, index_row):
    chunk_iota = lax.broadcasted_iota(jnp.int32, (rows, LANES), 0)
    left = []
    for s in range(8):
        value = jnp.broadcast_to(value_ref[s : s + 1, :], (rows, LANES))
        chunk = jnp.concatenate([wide(index_row(s)) >> 7] * (rows // 8), axis=0)
        left.append(jnp.where(chunk == chunk_iota, value, 0.0))
    high, low = split(jnp.concatenate(left, axis=1))
    summed = lax.dot_general(
        jnp.concatenate([high, low], axis=0).astype(BF16),
        marks,
        (((1,), (1,)), ((), ())),
        preferred_element_type=F32,
    )
    return summed[:rows] + summed[rows:]


def fill_table(table_ref, row, value):
    high = value.astype(BF16)
    low = (value - high.astype(F32)).astype(BF16)
    for half in range(2):
        columns = slice(half * LANES, (half + 1) * LANES)
        table_ref[half, row : row + NODE_ROWS, :] = high[:, columns]
        table_ref[2 + half, row : row + NODE_ROWS, :] = low[:, columns]


def mark(place_ref, once_ref, slot, indices):
    one, zero = jnp.ones((16, LANES), BF16), jnp.zeros((16, LANES), BF16)
    for n, index in enumerate(indices):
        column = small(index & (WIDE - 1))
        for row in range(0, WIDE, 16):
            match = column == place_ref[row : row + 16, :]
            once_ref[slot, n, row : row + 16, :] = jnp.where(match, one, zero)


def lookup(table_ref, first, groups, once_ref, slot, indices):
    once = jnp.concatenate([once_ref[slot, n] for n in range(len(indices))], axis=1)
    rows = slice(first * NODE_ROWS, (first + groups) * NODE_ROWS)
    found = sum(
        jnp.dot(
            jnp.concatenate([table_ref[plane, rows, :], table_ref[plane + 1, rows, :]], axis=1),
            once,
            preferred_element_type=F32,
        )
        for plane in (0, 2)
    )
    results = []
    for n, index in enumerate(indices):
        bits = bit_masks(index >> 8, 3)

        def piece(h, k):
            row = h * NODE_ROWS + 8 * k
            return found[row : row + 8, n * LANES : (n + 1) * LANES]

        results.append(
            [
                pick([lambda h=h: piece(h, k) for h in range(groups)], bits)
                for k in range(NODE_ROWS // 8)
            ]
        )
    return results


def face_common(perm_a, perm_b, product):
    both = perm_a + perm_b
    return 2.0 * perm_a * perm_b * product / (both * both)


def kernel(
    count,
    disp_hbm,
    adj_hbm,
    press_hbm,
    apress_hbm,
    youngs_hbm,
    perm_hbm,
    stiff_hbm,
    send_nodes_hbm,
    send_cells_hbm,
    elem_hbm,
    inner_hbm,
    cross_hbm,
    out_ref,
    disp_ref,
    adj_ref,
    press_ref,
    apress_ref,
    youngs_ref,
    perm_ref,
    stiff_ref,
    send_nodes_ref,
    send_cells_ref,
    elem_ref,
    inner_ref,
    cross_ref,
    cells_out,
    perms_out,
    nodes_out,
    cells_in,
    perms_in,
    nodes_in,
    back_out,
    back_in,
    term_a_ref,
    term_b_ref,
    edge_ref,
    face_ref,
    back_marks_ref,
    table_ref,
    place_ref,
    once_ref,
    edge_once_ref,
    state_ref,
    edge_state_ref,
    gradient_ref,
    cell_send,
    cell_recv,
    perm_send,
    perm_recv,
    node_send,
    node_recv,
    back_send,
    back_recv,
    stage_sem,
):
    me = lax.axis_index("dom")

    def on_axis(offset):
        return (me + offset >= 0) & (me + offset < count)

    barrier = pltpu.get_barrier_semaphore()
    neighbours = 0
    for offset in reversed(OFFSETS):

        @pl.when(on_axis(offset))
        def _():
            pl.semaphore_signal(
                barrier, inc=1, device_id=(me + offset,), device_id_type=MESH
            )

        neighbours = neighbours + on_axis(offset).astype(jnp.int32)

    staged = (
        (send_cells_hbm, send_cells_ref),
        (press_hbm, press_ref),
        (apress_hbm, apress_ref),
        (perm_hbm, perm_ref),
        (send_nodes_hbm, send_nodes_ref),
        (disp_hbm, disp_ref),
        (adj_hbm, adj_ref),
        (elem_hbm, elem_ref),
        (inner_hbm, inner_ref),
        (stiff_hbm, stiff_ref),
        (youngs_hbm, youngs_ref),
        (cross_hbm, cross_ref),
    )
    stages = [
        pltpu.make_async_copy(source, target, stage_sem.at[i])
        for i, (source, target) in enumerate(staged)
    ]
    for stage in stages:
        stage.start()

    def send(source, target, send_sem, recv_sem, j, offset):
        return pltpu.make_async_remote_copy(
            src_ref=source,
            dst_ref=target,
            send_sem=send_sem.at[j],
            recv_sem=recv_sem.at[j],
            device_id=(me + offset,),
            device_id_type=MESH,
        )

    def cell_copy(j):
        rows = pl.ds(j * CELL_ROWS, CELL_ROWS)
        return send(cells_out.at[rows], cells_in.at[rows], cell_send, cell_recv, j, -OFFSETS[j])

    def perm_copy(j):
        return send(perms_out.at[j], perms_in.at[j], perm_send, perm_recv, j, -OFFSETS[j])

    def node_copy(j):
        rows = pl.ds(j * NODE_ROWS, NODE_ROWS)
        return send(nodes_out.at[rows], nodes_in.at[rows], node_send, node_recv, j, -OFFSETS[j])

    def back_copy(j):
        return send(back_out.at[j], back_in.at[j], back_send, back_recv, j, OFFSETS[j])

    def each(sign, action):
        for j in reversed(range(NB)):
            pl.when(on_axis(sign * OFFSETS[j]))(lambda j=j: action(j))

    place = lax.broadcasted_iota(jnp.int32, (WIDE, LANES), 0)
    place_ref[...] = place.astype(F32).astype(BF16)
    gradient_ref[...] = jnp.zeros((OWN, LANES), F32)
    term_a_ref[...] = jnp.zeros((8, LANES), F32)
    term_b_ref[...] = jnp.zeros((8, LANES), F32)
    state_ref[...] = jnp.zeros(state_ref.shape, F32)
    for j in range(NB):

        @pl.when(jnp.logical_not(on_axis(OFFSETS[j])))
        def _():
            rows = slice(j * NODE_ROWS, (j + 1) * NODE_ROWS)
            nodes_in[rows, :] = jnp.zeros((NODE_ROWS, LANES), F32)

        @pl.when(jnp.logical_not(on_axis(-OFFSETS[j])))
        def _():
            back_in[j] = jnp.zeros((1, LANES), F32)

    for stage in stages:
        stage.wait()

    index = send_cells_ref[...]
    lanes, bits = index & 127, bit_masks(index >> 7, 4)
    for t in range(STEPS):
        cells_out[pl.ds(t, NB, stride=CELL_ROWS), :] = own_rows(press_ref, t, lanes, bits)
        cells_out[pl.ds(STEPS + t, NB, stride=CELL_ROWS), :] = own_rows(
            apress_ref, t, lanes, bits
        )
    permeability = own_perm(perm_ref, lanes, bits)
    for j in range(NB):
        perms_out[j] = permeability[j : j + 1, :]
    for h in range(OWN_GROUPS):
        columns = slice(h * WIDE, (h + 1) * WIDE)
        fill_table(
            table_ref,
            h * NODE_ROWS,
            jnp.concatenate([disp_ref[:, columns], adj_ref[:, columns]], axis=0),
        )
    for first in range(0, NB, GROUP):
        rows = [wide(send_nodes_ref[j : j + 1, :]) for j in range(first, first + GROUP)]
        slot = first // GROUP
        mark(place_ref, once_ref, slot, rows)
        found = lookup(table_ref, 0, OWN_GROUPS, once_ref, slot, rows)
        for j, pieces in zip(range(first, first + GROUP), found):
            for k, value in enumerate(pieces):
                row = j * NODE_ROWS + 8 * k
                nodes_out[row : row + 8, :] = value

    def send_states():
        pl.semaphore_wait(barrier, neighbours)

        def start_cells(j):
            cell_copy(j).start()
            perm_copy(j).start()

        each(-1, start_cells)
        each(-1, lambda j: node_copy(j).start())

    def gather_inner(block):
        base = pl.multiple_of(block * 16, 16)
        ends = []
        for side in range(2):
            index = inner_ref[pl.ds(base + side, 8, stride=2), :]
            lanes, bits = index & 127, bit_masks(index >> 7, 4)
            ends.append(
                (
                    [own_rows(press_ref, t, lanes, bits) for t in range(STEPS)],
                    [own_rows(apress_ref, t, lanes, bits) for t in range(STEPS)],
                    own_perm(perm_ref, lanes, bits),
                )
            )
        (pa, qa, ka), (pb, qb, kb) = ends
        product = sum((pa[t] - pb[t]) * (qa[t] - qb[t]) for t in range(STEPS))
        common = face_common(ka, kb, product)
        term_a_ref[...] = common * kb
        term_b_ref[...] = common * ka

    def scatter_inner(block):
        base = pl.multiple_of(block * 16, 16)
        gradient = gradient_ref[...]
        for side, term_ref in enumerate((term_a_ref, term_b_ref)):
            index_row = lambda s: inner_ref[pl.ds(base + 2 * s + side, 1), :]
            marks = lane_marks(place_ref, index_row)
            gradient = gradient + scatter_rows(marks, term_ref, OWN, index_row)
        gradient_ref[...] = gradient

    stiff_high, stiff_low = split(stiff_ref[...])
    stiff = jnp.concatenate([stiff_high, stiff_low, stiff_high], axis=1).astype(BF16)

    def element_rows(block, first):
        column = pl.multiple_of(block * LANES, LANES)
        return [
            wide(elem_ref[n : n + 1, pl.ds(column, LANES)]) for n in range(first, first + GROUP)
        ]

    def own_states(block, once, states, slot):
        for first in range(0, 8, GROUP):
            rows = element_rows(block, first)
            part = 2 * slot + first // GROUP
            mark(place_ref, once, part, rows)
            found = lookup(table_ref, 0, OWN_GROUPS, once, part, rows)
            for n, pieces in zip(range(first, first + GROUP), found):
                for k, value in enumerate(pieces):
                    row = n * PITCH + 8 * k
                    states[slot, row : row + 8, :] = value

    def ghost_states(block, slot):
        for first in range(0, 8, GROUP):
            rows = element_rows(block, first)
            part = 2 * slot + first // GROUP
            found = lookup(table_ref, OWN_GROUPS, GHOST_GROUPS, edge_once_ref, part, rows)
            for n, index, pieces in zip(range(first, first + GROUP), rows, found):
                outside = index >= OWN * LANES
                for k, value in enumerate(pieces):
                    row = n * PITCH + 8 * k
                    edge_state_ref[slot, row : row + 8, :] = jnp.where(
                        outside, value, edge_state_ref[slot, row : row + 8, :]
                    )

    def strain(block, states, slot):
        total = jnp.zeros((8, LANES), F32)
        for t in range(0, STEPS, 2):
            forward = jnp.concatenate(
                [
                    jnp.concatenate(
                        [states[slot, pl.ds(8 * c + u, 8, stride=PITCH), :] for c in range(3)],
                        axis=0,
                    )
                    for u in (t, t + 1)
                ],
                axis=1,
            )
            high, low = split(forward)
            stacked = jnp.concatenate([high, high, low], axis=0).astype(BF16)
            weighted = jnp.dot(stiff, stacked, preferred_element_type=F32)
            for u in range(2):
                for c in range(3):
                    adjoint = states[slot, pl.ds(24 + 8 * c + t + u, 8, stride=PITCH), :]
                    total = total + adjoint * weighted[
                        8 * c : 8 * c + 8, u * LANES : (u + 1) * LANES
                    ]
        summed = jnp.sum(total, axis=0, keepdims=True)
        out_ref[pl.ds(block, 1), :] = -youngs_ref[pl.ds(block, 1), :] * summed

    def shared_faces():
        index = cross_ref[pl.ds(0, 8, stride=2), :]
        lanes, bits = index & 127, bit_masks(index >> 7, 4)
        for t in range(STEPS):
            face_ref[t] = own_rows(press_ref, t, lanes, bits)
            face_ref[STEPS + t] = own_rows(apress_ref, t, lanes, bits)
        perm_a = own_perm(perm_ref, lanes, bits)
        index = cross_ref[pl.ds(1, 8, stride=2), :]
        ghost_lanes, ghost_bits = index & 127, bit_masks(index >> 7, 3)

        def ghost(row):
            return ghost_rows(
                lambda j: cells_in[j * CELL_ROWS + row : j * CELL_ROWS + row + 1, :],
                ghost_lanes,
                ghost_bits,
            )

        ghost_index = lambda s: cross_ref[2 * s + 1 : 2 * s + 2, :]
        own_index = lambda s: cross_ref[2 * s : 2 * s + 1, :]
        back_marks_ref[...] = lane_marks(place_ref, ghost_index)

        def wait_cells(j):
            cell_copy(j).wait_recv()
            perm_copy(j).wait_recv()

        each(1, wait_cells)
        product = jnp.zeros((8, LANES), F32)
        for t in range(STEPS):
            product = product + (face_ref[t] - ghost(t)) * (
                face_ref[STEPS + t] - ghost(STEPS + t)
            )
        perm_b = ghost_rows(lambda j: perms_in[j], ghost_lanes, ghost_bits)
        common = face_common(perm_a, perm_b, product)
        edge_ref[0] = common * perm_b
        edge_ref[1] = common * perm_a
        returned = scatter_rows(back_marks_ref[...], edge_ref.at[1], NB, ghost_index)
        for j in range(NB):
            back_out[j] = returned[j : j + 1, :]
        each(1, lambda j: back_copy(j).start())
        gradient_ref[...] += scatter_rows(
            lane_marks(place_ref, own_index), edge_ref.at[0], OWN, own_index
        )

    place_z = lax.rem(me, SPAN) // 2
    early = place_z < SPAN // 4
    row_start = (me >= ROW) & (lax.rem(me, ROW) < SPAN)
    send_at = jnp.where(early, EARLIEST - place_z + row_start.astype(jnp.int32), 0)
    cross_at = jnp.minimum(send_at + CROSS_AFTER, CELL_BLOCKS)

    @pl.loop(0, CELL_BLOCKS)
    def _(step):
        pl.when(step == send_at)(send_states)
        pl.when(step == cross_at)(shared_faces)
        before = jnp.maximum(step - 1, 0)
        strain(2 * before, state_ref, 0)
        strain(2 * before + 1, state_ref, 1)
        scatter_inner(before)
        own_states(2 * step, once_ref, state_ref, 0)
        own_states(2 * step + 1, once_ref, state_ref, 1)
        gather_inner(step)

    strain(INNER_BLOCKS - 2, state_ref, 0)
    strain(INNER_BLOCKS - 1, state_ref, 1)
    scatter_inner(CELL_BLOCKS - 1)
    for slot in range(EDGE_BLOCKS):
        own_states(INNER_BLOCKS + slot, edge_once_ref, edge_state_ref, slot)
    pl.when(send_at == CELL_BLOCKS)(send_states)
    pl.when(cross_at == CELL_BLOCKS)(shared_faces)

    each(1, lambda j: node_copy(j).wait_recv())
    for h in range(GHOST_GROUPS):
        row = (OWN_GROUPS + h) * NODE_ROWS
        ghosts = [
            nodes_in[j * NODE_ROWS : (j + 1) * NODE_ROWS, :] for j in (2 * h, 2 * h + 1)
        ]
        fill_table(table_ref, row, jnp.concatenate(ghosts, axis=1))
    for slot in range(EDGE_BLOCKS):
        ghost_states(INNER_BLOCKS + slot, slot)
    for slot in range(EDGE_BLOCKS):
        strain(INNER_BLOCKS + slot, edge_state_ref, slot)

    cell_index = lambda s: send_cells_ref[s : s + 1, :]
    back_marks_ref[...] = lane_marks(place_ref, cell_index)
    each(-1, lambda j: back_copy(j).wait_recv())
    edge_ref[0] = jnp.concatenate([back_in[j] for j in range(NB)], axis=0)
    out_ref[OWN:, :] = gradient_ref[...] + scatter_rows(
        back_marks_ref[...], edge_ref.at[0], OWN, cell_index
    )
    each(-1, lambda j: cell_copy(j).wait_send())
    each(-1, lambda j: perm_copy(j).wait_send())
    each(-1, lambda j: node_copy(j).wait_send())
    each(1, lambda j: back_copy(j).wait_send())


def on_device(
    displacement,
    adjoint_disp,
    pressure,
    adjoint_pressure,
    youngs,
    permeability,
    stiffness,
    send_nodes,
    send_cells,
    elem_nodes,
    inner_faces,
    cross_faces,
):
    count = lax.axis_size("dom")

    def components(value):
        return value.transpose(1, 0, 2).reshape(24, -1)

    def interleaved(value):
        return value.reshape(2, -1, LANES).transpose(1, 0, 2).reshape(-1, LANES)

    vmem = pl.BlockSpec(memory_space=pltpu.VMEM)
    gradients = pl.pallas_call(
        functools.partial(kernel, count),
        out_shape=pltpu.VMEM((2 * OWN, LANES), F32),
        in_specs=[pl.BlockSpec(memory_space=pltpu.HBM)] * 12,
        out_specs=vmem,
        scratch_shapes=[
            pltpu.VMEM((24, OWN * LANES), F32),
            pltpu.VMEM((24, OWN * LANES), F32),
            pltpu.VMEM((STEPS, OWN * LANES), F32),
            pltpu.VMEM((STEPS, OWN * LANES), F32),
            pltpu.VMEM((OWN, LANES), F32),
            pltpu.VMEM((OWN, LANES), F32),
            pltpu.VMEM((24, 24), F32),
            pltpu.VMEM((NB, LANES), jnp.int32),
            pltpu.VMEM((NB, LANES), jnp.int32),
            pltpu.VMEM((8, OWN * LANES), jnp.int32),
            pltpu.VMEM((16 * CELL_BLOCKS, LANES), jnp.int32),
            pltpu.VMEM((16, LANES), jnp.int32),
            pltpu.VMEM((NB * CELL_ROWS, LANES), F32),
            pltpu.VMEM((NB, 1, LANES), F32),
            pltpu.VMEM((NB * NODE_ROWS, LANES), F32),
            pltpu.VMEM((NB * CELL_ROWS, LANES), F32),
            pltpu.VMEM((NB, 1, LANES), F32),
            pltpu.VMEM((NB * NODE_ROWS, LANES), F32),
            pltpu.VMEM((NB, 1, LANES), F32),
            pltpu.VMEM((NB, 1, LANES), F32),
            pltpu.VMEM((8, LANES), F32),
            pltpu.VMEM((8, LANES), F32),
            pltpu.VMEM((2, 8, LANES), F32),
            pltpu.VMEM((2 * STEPS, 8, LANES), F32),
            pltpu.VMEM((LANES, 8 * LANES), BF16),
            pltpu.VMEM((4, (OWN_GROUPS + GHOST_GROUPS) * NODE_ROWS, LANES), BF16),
            pltpu.VMEM((WIDE, LANES), BF16),
            pltpu.VMEM((4, GROUP, WIDE, LANES), BF16),
            pltpu.VMEM((2 * EDGE_BLOCKS, GROUP, WIDE, LANES), BF16),
            pltpu.VMEM((2, 8 * PITCH, LANES), F32),
            pltpu.VMEM((EDGE_BLOCKS, 8 * PITCH, LANES), F32),
            pltpu.VMEM((OWN, LANES), F32),
        ]
        + [pltpu.SemaphoreType.DMA((NB,))] * 8
        + [pltpu.SemaphoreType.DMA((12,))],
        compiler_params=pltpu.CompilerParams(collective_id=0, has_side_effects=True),
    )(
        components(displacement),
        components(adjoint_disp),
        pressure,
        adjoint_pressure,
        youngs.reshape(OWN, LANES),
        permeability.reshape(OWN, LANES),
        stiffness,
        send_nodes,
        send_cells,
        elem_nodes,
        interleaved(inner_faces),
        interleaved(cross_faces),
    )
    return gradients[:OWN].reshape(-1), gradients[OWN:].reshape(-1)


def solution(mesh):
    in_specs = (
        P(None, None, "dom"),
        P(None, None, "dom"),
        P(None, "dom"),
        P(None, "dom"),
        P("dom"),
        P("dom"),
        P(),
        P(None, "dom"),
        P(None, "dom"),
        P(None, "dom"),
        P(None, "dom"),
        P(None, "dom"),
    )
    return jax.shard_map(
        on_device,
        mesh=mesh,
        in_specs=in_specs,
        out_specs=(P("dom"), P("dom")),
        check_vma=False,
    )
```

```python
import functools

import jax
import jax.numpy as jnp
from jax import lax
from jax.experimental import pallas as pl
from jax.experimental.pallas import tpu as pltpu
from jax.sharding import PartitionSpec as P

OFFSETS = (1, -1, 2, -2, 4, -4, 8, -8)
MESH = pl.DeviceIdType.MESH
F32 = jnp.float32
BF16 = jnp.bfloat16
LANES = 128
STEPS = 8
OWN = 16
NB = 8
CELL_ROWS = 16
NODE_ROWS = 48
CELL_BLOCKS = 6
INNER_BLOCKS = 12
EDGE_BLOCKS = 4
WIDE = 256
OWN_GROUPS = 8
GHOST_GROUPS = 4
GROUP = 4
PITCH = 56
SPAN = 16
ROW = 64
EARLIEST = 4
CROSS_AFTER = 4


def take(source, lanes):
    return jnp.take_along_axis(source, lanes, axis=1, mode="promise_in_bounds")


def pick(values, bits):
    if len(values) == 1:
        return values[0]()
    half = len(values) // 2
    top = bits[half.bit_length() - 1]
    low = pick(values[:half], bits)
    high = pick(values[half:], bits)
    return jnp.where(top, high, low)


def wide(row):
    return jnp.broadcast_to(row, (8, LANES))


def bit_masks(chunk, count):
    return [(chunk & (1 << bit)) != 0 for bit in range(count)]


def own_rows(ref, row, lanes, bits):
    return pick(
        [
            lambda h=h: take(wide(ref[row : row + 1, h * LANES : (h + 1) * LANES]), lanes)
            for h in range(OWN)
        ],
        bits,
    )


def own_perm(ref, lanes, bits):
    return pick(
        [lambda h=h: take(wide(ref[h : h + 1, :]), lanes) for h in range(OWN)], bits
    )


def ghost_rows(rows, lanes, bits):
    return pick([lambda j=j: take(wide(rows(j)), lanes) for j in range(NB)], bits)


def split(value):
    high = value.astype(BF16).astype(F32)
    return high, value - high


def small(column):
    column = column.astype(F32)
    return jnp.concatenate([column, column], axis=0).astype(BF16)


def lane_marks(place_ref, index_row):
    one, zero = jnp.ones((16, LANES), BF16), jnp.zeros((16, LANES), BF16)
    columns = []
    for s in range(8):
        lane = small(wide(index_row(s)) & (LANES - 1))
        columns.append(
            jnp.concatenate(
                [
                    jnp.where(lane == place_ref[row : row + 16, :], one, zero)
                    for row in range(0, LANES, 16)
                ],
                axis=0,
            )
        )
    return jnp.concatenate(columns, axis=1)


def scatter_rows(marks, value_ref, rows, index_row, faces=range(8)):
    chunk_iota = lax.broadcasted_iota(jnp.int32, (rows, LANES), 0)
    left = []
    for s in faces:
        value = jnp.broadcast_to(value_ref[s : s + 1, :], (rows, LANES))
        chunk = jnp.concatenate([wide(index_row(s)) >> 7] * (rows // 8), axis=0)
        left.append(jnp.where(chunk == chunk_iota, value, 0.0))
    high, low = split(jnp.concatenate(left, axis=1))
    summed = lax.dot_general(
        jnp.concatenate([high, low], axis=0).astype(BF16),
        marks,
        (((1,), (1,)), ((), ())),
        preferred_element_type=F32,
    )
    return summed[:rows] + summed[rows:]


def fill_table(table_ref, row, value):
    high = value.astype(BF16)
    low = (value - high.astype(F32)).astype(BF16)
    for half in range(2):
        columns = slice(half * LANES, (half + 1) * LANES)
        table_ref[half, row : row + NODE_ROWS, :] = high[:, columns]
        table_ref[2 + half, row : row + NODE_ROWS, :] = low[:, columns]


def mark(place_ref, once_ref, slot, indices):
    one, zero = jnp.ones((16, LANES), BF16), jnp.zeros((16, LANES), BF16)
    for n, index in enumerate(indices):
        column = small(index & (WIDE - 1))
        for row in range(0, WIDE, 16):
            match = column == place_ref[row : row + 16, :]
            once_ref[slot, n, row : row + 16, :] = jnp.where(match, one, zero)


def lookup(table_ref, first, groups, once_ref, slot, indices):
    once = jnp.concatenate([once_ref[slot, n] for n in range(len(indices))], axis=1)
    rows = slice(first * NODE_ROWS, (first + groups) * NODE_ROWS)
    found = sum(
        jnp.dot(
            jnp.concatenate([table_ref[plane, rows, :], table_ref[plane + 1, rows, :]], axis=1),
            once,
            preferred_element_type=F32,
        )
        for plane in (0, 2)
    )
    results = []
    for n, index in enumerate(indices):
        bits = bit_masks(index >> 8, 3)

        def piece(h, k):
            row = h * NODE_ROWS + 8 * k
            return found[row : row + 8, n * LANES : (n + 1) * LANES]

        results.append(
            [
                pick([lambda h=h: piece(h, k) for h in range(groups)], bits)
                for k in range(NODE_ROWS // 8)
            ]
        )
    return results


def face_common(perm_a, perm_b, product):
    both = perm_a + perm_b
    return 2.0 * perm_a * perm_b * product / (both * both)


def kernel(
    count,
    disp_hbm,
    adj_hbm,
    press_hbm,
    apress_hbm,
    youngs_hbm,
    perm_hbm,
    stiff_hbm,
    send_nodes_hbm,
    send_cells_hbm,
    elem_hbm,
    inner_hbm,
    cross_hbm,
    out_ref,
    disp_ref,
    adj_ref,
    press_ref,
    apress_ref,
    youngs_ref,
    perm_ref,
    stiff_ref,
    send_nodes_ref,
    send_cells_ref,
    elem_ref,
    inner_ref,
    cross_ref,
    cells_out,
    perms_out,
    nodes_out,
    cells_in,
    perms_in,
    nodes_in,
    back_out,
    back_in,
    term_a_ref,
    term_b_ref,
    edge_ref,
    face_ref,
    back_marks_ref,
    table_ref,
    place_ref,
    once_ref,
    edge_once_ref,
    state_ref,
    edge_state_ref,
    gradient_ref,
    cell_send,
    cell_recv,
    perm_send,
    perm_recv,
    node_send,
    node_recv,
    back_send,
    back_recv,
    stage_sem,
):
    me = lax.axis_index("dom")

    def on_axis(offset):
        return (me + offset >= 0) & (me + offset < count)

    barrier = pltpu.get_barrier_semaphore()
    neighbours = 0
    for offset in reversed(OFFSETS):

        @pl.when(on_axis(offset))
        def _():
            pl.semaphore_signal(
                barrier, inc=1, device_id=(me + offset,), device_id_type=MESH
            )

        neighbours = neighbours + on_axis(offset).astype(jnp.int32)

    staged = (
        (send_cells_hbm, send_cells_ref),
        (press_hbm, press_ref),
        (apress_hbm, apress_ref),
        (perm_hbm, perm_ref),
        (send_nodes_hbm, send_nodes_ref),
        (disp_hbm, disp_ref),
        (adj_hbm, adj_ref),
        (elem_hbm, elem_ref),
        (inner_hbm, inner_ref),
        (stiff_hbm, stiff_ref),
        (youngs_hbm, youngs_ref),
        (cross_hbm, cross_ref),
    )
    stages = [
        pltpu.make_async_copy(source, target, stage_sem.at[i])
        for i, (source, target) in enumerate(staged)
    ]
    for stage in stages:
        stage.start()

    def send(source, target, send_sem, recv_sem, j, offset):
        return pltpu.make_async_remote_copy(
            src_ref=source,
            dst_ref=target,
            send_sem=send_sem.at[j],
            recv_sem=recv_sem.at[j],
            device_id=(me + offset,),
            device_id_type=MESH,
        )

    def cell_copy(j):
        rows = pl.ds(j * CELL_ROWS, CELL_ROWS)
        return send(cells_out.at[rows], cells_in.at[rows], cell_send, cell_recv, j, -OFFSETS[j])

    def perm_copy(j):
        return send(perms_out.at[j], perms_in.at[j], perm_send, perm_recv, j, -OFFSETS[j])

    def node_copy(j):
        rows = pl.ds(j * NODE_ROWS, NODE_ROWS)
        return send(nodes_out.at[rows], nodes_in.at[rows], node_send, node_recv, j, -OFFSETS[j])

    def back_copy(j):
        return send(back_out.at[j], back_in.at[j], back_send, back_recv, j, OFFSETS[j])

    def each(sign, action):
        for j in reversed(range(NB)):
            pl.when(on_axis(sign * OFFSETS[j]))(lambda j=j: action(j))

    place = lax.broadcasted_iota(jnp.int32, (WIDE, LANES), 0)
    place_ref[...] = place.astype(F32).astype(BF16)
    gradient_ref[...] = jnp.zeros((OWN, LANES), F32)
    term_a_ref[...] = jnp.zeros((8, LANES), F32)
    term_b_ref[...] = jnp.zeros((8, LANES), F32)
    state_ref[...] = jnp.zeros(state_ref.shape, F32)
    for j in range(NB):

        @pl.when(jnp.logical_not(on_axis(OFFSETS[j])))
        def _():
            rows = slice(j * NODE_ROWS, (j + 1) * NODE_ROWS)
            nodes_in[rows, :] = jnp.zeros((NODE_ROWS, LANES), F32)

        @pl.when(jnp.logical_not(on_axis(-OFFSETS[j])))
        def _():
            back_in[j] = jnp.zeros((1, LANES), F32)

    for stage in stages:
        stage.wait()

    index = send_cells_ref[...]
    lanes, bits = index & 127, bit_masks(index >> 7, 4)
    for t in range(STEPS):
        cells_out[pl.ds(t, NB, stride=CELL_ROWS), :] = own_rows(press_ref, t, lanes, bits)
        cells_out[pl.ds(STEPS + t, NB, stride=CELL_ROWS), :] = own_rows(
            apress_ref, t, lanes, bits
        )
    permeability = own_perm(perm_ref, lanes, bits)
    for j in range(NB):
        perms_out[j] = permeability[j : j + 1, :]
    for h in range(OWN_GROUPS):
        columns = slice(h * WIDE, (h + 1) * WIDE)
        fill_table(
            table_ref,
            h * NODE_ROWS,
            jnp.concatenate([disp_ref[:, columns], adj_ref[:, columns]], axis=0),
        )
    for first in range(0, NB, GROUP):
        rows = [wide(send_nodes_ref[j : j + 1, :]) for j in range(first, first + GROUP)]
        slot = first // GROUP
        mark(place_ref, once_ref, slot, rows)
        found = lookup(table_ref, 0, OWN_GROUPS, once_ref, slot, rows)
        for j, pieces in zip(range(first, first + GROUP), found):
            for k, value in enumerate(pieces):
                row = j * NODE_ROWS + 8 * k
                nodes_out[row : row + 8, :] = value

    def send_states():
        pl.semaphore_wait(barrier, neighbours)

        def start_cells(j):
            cell_copy(j).start()
            perm_copy(j).start()

        each(-1, start_cells)
        each(-1, lambda j: node_copy(j).start())

    def gather_inner(block):
        base = pl.multiple_of(block * 16, 16)
        ends = []
        for side in range(2):
            index = inner_ref[pl.ds(base + side, 8, stride=2), :]
            lanes, bits = index & 127, bit_masks(index >> 7, 4)
            ends.append(
                (
                    [own_rows(press_ref, t, lanes, bits) for t in range(STEPS)],
                    [own_rows(apress_ref, t, lanes, bits) for t in range(STEPS)],
                    own_perm(perm_ref, lanes, bits),
                )
            )
        (pa, qa, ka), (pb, qb, kb) = ends
        product = sum((pa[t] - pb[t]) * (qa[t] - qb[t]) for t in range(STEPS))
        common = face_common(ka, kb, product)
        term_a_ref[...] = common * kb
        term_b_ref[...] = common * ka

    def scatter_inner(block):
        base = pl.multiple_of(block * 16, 16)
        gradient = gradient_ref[...]
        for side, term_ref in enumerate((term_a_ref, term_b_ref)):
            index_row = lambda s: inner_ref[pl.ds(base + 2 * s + side, 1), :]
            marks = lane_marks(place_ref, index_row)
            gradient = gradient + scatter_rows(marks, term_ref, OWN, index_row)
        gradient_ref[...] = gradient

    stiff_high, stiff_low = split(stiff_ref[...])
    stiff = jnp.concatenate([stiff_high, stiff_low, stiff_high], axis=1).astype(BF16)

    def element_rows(block, first):
        column = pl.multiple_of(block * LANES, LANES)
        return [
            wide(elem_ref[n : n + 1, pl.ds(column, LANES)]) for n in range(first, first + GROUP)
        ]

    def own_states(block, once, states, slot):
        for first in range(0, 8, GROUP):
            rows = element_rows(block, first)
            part = 2 * slot + first // GROUP
            mark(place_ref, once, part, rows)
            found = lookup(table_ref, 0, OWN_GROUPS, once, part, rows)
            for n, pieces in zip(range(first, first + GROUP), found):
                for k, value in enumerate(pieces):
                    row = n * PITCH + 8 * k
                    states[slot, row : row + 8, :] = value

    def ghost_states(block, slot):
        for first in range(0, 8, GROUP):
            rows = element_rows(block, first)
            part = 2 * slot + first // GROUP
            found = lookup(table_ref, OWN_GROUPS, GHOST_GROUPS, edge_once_ref, part, rows)
            for n, index, pieces in zip(range(first, first + GROUP), rows, found):
                outside = index >= OWN * LANES
                for k, value in enumerate(pieces):
                    row = n * PITCH + 8 * k
                    edge_state_ref[slot, row : row + 8, :] = jnp.where(
                        outside, value, edge_state_ref[slot, row : row + 8, :]
                    )

    def strain(block, states, slot):
        total = jnp.zeros((8, LANES), F32)
        for t in range(0, STEPS, 2):
            forward = jnp.concatenate(
                [
                    jnp.concatenate(
                        [states[slot, pl.ds(8 * c + u, 8, stride=PITCH), :] for c in range(3)],
                        axis=0,
                    )
                    for u in (t, t + 1)
                ],
                axis=1,
            )
            high, low = split(forward)
            stacked = jnp.concatenate([high, high, low], axis=0).astype(BF16)
            weighted = jnp.dot(stiff, stacked, preferred_element_type=F32)
            for u in range(2):
                for c in range(3):
                    adjoint = states[slot, pl.ds(24 + 8 * c + t + u, 8, stride=PITCH), :]
                    total = total + adjoint * weighted[
                        8 * c : 8 * c + 8, u * LANES : (u + 1) * LANES
                    ]
        summed = jnp.sum(total, axis=0, keepdims=True)
        out_ref[pl.ds(block, 1), :] = -youngs_ref[pl.ds(block, 1), :] * summed

    def shared_faces():
        index = cross_ref[pl.ds(0, 8, stride=2), :]
        lanes, bits = index & 127, bit_masks(index >> 7, 4)
        for t in range(STEPS):
            face_ref[t] = own_rows(press_ref, t, lanes, bits)
            face_ref[STEPS + t] = own_rows(apress_ref, t, lanes, bits)
        perm_a = own_perm(perm_ref, lanes, bits)
        index = cross_ref[pl.ds(1, 8, stride=2), :]
        ghost_lanes, ghost_bits = index & 127, bit_masks(index >> 7, 3)

        def ghost(row):
            return ghost_rows(
                lambda j: cells_in[j * CELL_ROWS + row : j * CELL_ROWS + row + 1, :],
                ghost_lanes,
                ghost_bits,
            )

        ghost_index = lambda s: cross_ref[2 * s + 1 : 2 * s + 2, :]
        own_index = lambda s: cross_ref[2 * s : 2 * s + 1, :]
        back_marks_ref[...] = lane_marks(place_ref, ghost_index)

        def wait_cells(j):
            cell_copy(j).wait_recv()
            perm_copy(j).wait_recv()

        each(1, wait_cells)
        product = jnp.zeros((8, LANES), F32)
        for t in range(STEPS):
            product = product + (face_ref[t] - ghost(t)) * (
                face_ref[STEPS + t] - ghost(STEPS + t)
            )
        perm_b = ghost_rows(lambda j: perms_in[j], ghost_lanes, ghost_bits)
        common = face_common(perm_a, perm_b, product)
        edge_ref[0] = common * perm_b
        edge_ref[1] = common * perm_a
        returned = scatter_rows(back_marks_ref[...], edge_ref.at[1], NB, ghost_index)
        for j in range(NB):
            back_out[j] = returned[j : j + 1, :]
        each(1, lambda j: back_copy(j).start())
        gradient_ref[...] += scatter_rows(
            lane_marks(place_ref, own_index), edge_ref.at[0], OWN, own_index
        )

    place_z = lax.rem(me, SPAN) // 2
    early = place_z < SPAN // 4
    row_start = (me >= ROW) & (lax.rem(me, ROW) < SPAN)
    send_at = jnp.where(early, EARLIEST - place_z + row_start.astype(jnp.int32), 0)
    cross_at = jnp.minimum(send_at + CROSS_AFTER, CELL_BLOCKS)

    @pl.loop(0, CELL_BLOCKS)
    def _(step):
        pl.when(step == send_at)(send_states)
        pl.when(step == cross_at)(shared_faces)
        before = jnp.maximum(step - 1, 0)
        strain(2 * before, state_ref, 0)
        strain(2 * before + 1, state_ref, 1)
        scatter_inner(before)
        own_states(2 * step, once_ref, state_ref, 0)
        own_states(2 * step + 1, once_ref, state_ref, 1)
        gather_inner(step)

    strain(INNER_BLOCKS - 2, state_ref, 0)
    strain(INNER_BLOCKS - 1, state_ref, 1)
    scatter_inner(CELL_BLOCKS - 1)
    for slot in range(EDGE_BLOCKS):
        own_states(INNER_BLOCKS + slot, edge_once_ref, edge_state_ref, slot)
    pl.when(send_at == CELL_BLOCKS)(send_states)
    pl.when(cross_at == CELL_BLOCKS)(shared_faces)

    each(1, lambda j: node_copy(j).wait_recv())
    for h in range(GHOST_GROUPS):
        row = (OWN_GROUPS + h) * NODE_ROWS
        ghosts = [
            nodes_in[j * NODE_ROWS : (j + 1) * NODE_ROWS, :] for j in (2 * h, 2 * h + 1)
        ]
        fill_table(table_ref, row, jnp.concatenate(ghosts, axis=1))
    for slot in range(EDGE_BLOCKS):
        ghost_states(INNER_BLOCKS + slot, slot)
    for slot in range(EDGE_BLOCKS):
        strain(INNER_BLOCKS + slot, edge_state_ref, slot)

    each(-1, lambda j: cell_copy(j).wait_send())
    each(-1, lambda j: perm_copy(j).wait_send())
    each(-1, lambda j: node_copy(j).wait_send())
    each(1, lambda j: back_copy(j).wait_send())
    cell_index = lambda s: send_cells_ref[s : s + 1, :]
    back_marks_ref[...] = lane_marks(place_ref, cell_index)
    gradient = gradient_ref[...]
    for slots in (range(NB - 2), range(NB - 2, NB)):
        for j in slots:
            pl.when(on_axis(-OFFSETS[j]))(lambda j=j: back_copy(j).wait_recv())
        for j in slots:
            edge_ref[0, j : j + 1, :] = back_in[j]
        columns = slice(slots[0] * LANES, (slots[-1] + 1) * LANES)
        gradient = gradient + scatter_rows(
            back_marks_ref[:, columns], edge_ref.at[0], OWN, cell_index, slots
        )
    out_ref[OWN:, :] = gradient


def on_device(
    displacement,
    adjoint_disp,
    pressure,
    adjoint_pressure,
    youngs,
    permeability,
    stiffness,
    send_nodes,
    send_cells,
    elem_nodes,
    inner_faces,
    cross_faces,
):
    count = lax.axis_size("dom")

    def components(value):
        return value.transpose(1, 0, 2).reshape(24, -1)

    def interleaved(value):
        return value.reshape(2, -1, LANES).transpose(1, 0, 2).reshape(-1, LANES)

    vmem = pl.BlockSpec(memory_space=pltpu.VMEM)
    gradients = pl.pallas_call(
        functools.partial(kernel, count),
        out_shape=pltpu.VMEM((2 * OWN, LANES), F32),
        in_specs=[pl.BlockSpec(memory_space=pltpu.HBM)] * 12,
        out_specs=vmem,
        scratch_shapes=[
            pltpu.VMEM((24, OWN * LANES), F32),
            pltpu.VMEM((24, OWN * LANES), F32),
            pltpu.VMEM((STEPS, OWN * LANES), F32),
            pltpu.VMEM((STEPS, OWN * LANES), F32),
            pltpu.VMEM((OWN, LANES), F32),
            pltpu.VMEM((OWN, LANES), F32),
            pltpu.VMEM((24, 24), F32),
            pltpu.VMEM((NB, LANES), jnp.int32),
            pltpu.VMEM((NB, LANES), jnp.int32),
            pltpu.VMEM((8, OWN * LANES), jnp.int32),
            pltpu.VMEM((16 * CELL_BLOCKS, LANES), jnp.int32),
            pltpu.VMEM((16, LANES), jnp.int32),
            pltpu.VMEM((NB * CELL_ROWS, LANES), F32),
            pltpu.VMEM((NB, 1, LANES), F32),
            pltpu.VMEM((NB * NODE_ROWS, LANES), F32),
            pltpu.VMEM((NB * CELL_ROWS, LANES), F32),
            pltpu.VMEM((NB, 1, LANES), F32),
            pltpu.VMEM((NB * NODE_ROWS, LANES), F32),
            pltpu.VMEM((NB, 1, LANES), F32),
            pltpu.VMEM((NB, 1, LANES), F32),
            pltpu.VMEM((8, LANES), F32),
            pltpu.VMEM((8, LANES), F32),
            pltpu.VMEM((2, 8, LANES), F32),
            pltpu.VMEM((2 * STEPS, 8, LANES), F32),
            pltpu.VMEM((LANES, 8 * LANES), BF16),
            pltpu.VMEM((4, (OWN_GROUPS + GHOST_GROUPS) * NODE_ROWS, LANES), BF16),
            pltpu.VMEM((WIDE, LANES), BF16),
            pltpu.VMEM((4, GROUP, WIDE, LANES), BF16),
            pltpu.VMEM((2 * EDGE_BLOCKS, GROUP, WIDE, LANES), BF16),
            pltpu.VMEM((2, 8 * PITCH, LANES), F32),
            pltpu.VMEM((EDGE_BLOCKS, 8 * PITCH, LANES), F32),
            pltpu.VMEM((OWN, LANES), F32),
        ]
        + [pltpu.SemaphoreType.DMA((NB,))] * 8
        + [pltpu.SemaphoreType.DMA((12,))],
        compiler_params=pltpu.CompilerParams(collective_id=0, has_side_effects=True),
    )(
        components(displacement),
        components(adjoint_disp),
        pressure,
        adjoint_pressure,
        youngs.reshape(OWN, LANES),
        permeability.reshape(OWN, LANES),
        stiffness,
        send_nodes,
        send_cells,
        elem_nodes,
        interleaved(inner_faces),
        interleaved(cross_faces),
    )
    return gradients[:OWN].reshape(-1), gradients[OWN:].reshape(-1)


def solution(mesh):
    in_specs = (
        P(None, None, "dom"),
        P(None, None, "dom"),
        P(None, "dom"),
        P(None, "dom"),
        P("dom"),
        P("dom"),
        P(),
        P(None, "dom"),
        P(None, "dom"),
        P(None, "dom"),
        P(None, "dom"),
        P(None, "dom"),
    )
    return jax.shard_map(
        on_device,
        mesh=mesh,
        in_specs=in_specs,
        out_specs=(P("dom"), P("dom")),
        check_vma=False,
    )
```
